128 devices in a mesh: row: 16 (over y, z_lo, core), col: 8 (over z_hi, x).
Axes of the slice: x: 4, y: 4, z: 4 (z_hi: 2, z_lo: 2; z = z_hi * 2 + z_lo), core: 2. Of those that a mesh axis runs over, the one named last changes fastest.
Arguments:
- points: float32 [64, 32768], P(None, ('row', 'col')), may hold values from -6 to 6
- labels: int32 [256], P(('row', 'col')), may hold values from 0 to 1
- solution: float32 [32768], P(('row', 'col')), may hold values from -6 to 6
- residual: float32 [32768], P(('row', 'col')), may hold values from -6 to 6
- direction: float32 [32768], P(('row', 'col')), may hold values from -6 to 6
- len_low: float32 [64], replicated, may hold values from 0.75 to 40
- len_high: float32 [64], replicated, may hold values from 0.9 to 40
- variances: float32 [2], replicated, may hold values from 0.5 to 2
- nugget: float32 [2], replicated, may hold values from 0.3 to 1.5
- coupling: float32 [1], replicated, may hold values from 0.6 to 1.6
Outputs:
- solution_next: float32 [32768], P(('row', 'col'))
- residual_next: float32 [32768], P(('row', 'col'))
- direction_next: float32 [32768], P(('row', 'col'))
The draws below stay inside these ranges and needn't reach their ends.
All inputs are finite; a program needn't handle non-finite values.
Results may differ from the reference program's by a relative error of at most 0.00027.
Values sent between devices are 32-bit elements; how exact they have to be, the bound alone decides.
A program may use at most 64 MiB of HBM per device.

```python
import math
import jax
import jax.numpy as jnp
from jax import lax

FEATURES = 64
NPTS = 32768
BLOCKS = 256


def draw_lengths(key, salt, short_lo, short_hi, long_lo, long_hi):
    ranking = jax.random.permutation(jax.random.fold_in(key, salt + 1), FEATURES)
    relevant = ranking < 6
    first_draw = jax.random.uniform(jax.random.fold_in(key, salt + 2), (FEATURES,), jnp.float32)
    second_draw = jax.random.uniform(jax.random.fold_in(key, salt + 3), (FEATURES,), jnp.float32)
    short_scale = jnp.exp(jnp.log(short_lo) + first_draw * (jnp.log(short_hi) - jnp.log(short_lo)))
    long_scale = jnp.exp(jnp.log(long_lo) + second_draw * (jnp.log(long_hi) - jnp.log(long_lo)))
    return jnp.where(relevant, short_scale, long_scale).astype(jnp.float32)


def draw_len_low(key, part):
    return draw_lengths(key, 100, 0.75, 1.4, 15.0, 40.0)


def draw_len_high(key, part):
    return draw_lengths(key, 200, 0.9, 1.7, 15.0, 40.0)


def draw_points(key, part):
    normals = jax.random.normal(jax.random.fold_in(key, 31), (FEATURES, NPTS), jnp.float32)
    return jnp.clip(normals, -6.0, 6.0).astype(jnp.float32)


def place_ends(drawn, key, low, high):
    place = [jax.random.randint(jax.random.fold_in(key, axis), (), 0, length) for axis, length in enumerate(drawn.shape)]
    widest = drawn.shape.index(max(drawn.shape))
    next_to = place[:widest] + [(place[widest] + 1) % drawn.shape[widest]] + place[widest + 1:]
    return drawn.at[tuple(place)].set(low).at[tuple(next_to)].set(high)


def block_levels(key, extent, split, low, high):
    level, own = 1.0, jax.random.fold_in(key, 6)
    for axis_at, shards_of in split:
        heights = jnp.exp(jax.random.uniform(jax.random.fold_in(own, axis_at), (shards_of,), jnp.float32, low / len(split), high / len(split)))
        level = level * jnp.repeat(heights, extent[axis_at] // shards_of).reshape([-1 if axis == axis_at else 1 for axis in range(len(extent))])
    return level


def noise(key, extent, deviation, reach, split=(), kind=jnp.bfloat16):
    entries = jax.random.normal(key, extent, jnp.float32) * deviation
    if len(split) > 0:
        entries = block_levels(key, extent, split, -0.22, 0.18) * entries
    return jnp.clip(entries, min=-reach, max=reach).astype(kind)


def setup_inputs(seed: int = 0) -> dict:
    splits = jax.random.split(jax.random.key(seed), 11)
    return {
        "points": draw_points(jax.random.fold_in(splits[10], 71), 0),
        "labels": place_ends(jax.random.randint(splits[1], (BLOCKS,), 0, 2), jax.random.fold_in(splits[1], 1), 0, 1).astype(jnp.int32),
        "solution": noise(splits[2], (NPTS,), 1.0, 6.0, ((0, 128),), jnp.float32),
        "residual": noise(splits[3], (NPTS,), 1.0, 6.0, ((0, 128),), jnp.float32),
        "direction": noise(splits[4], (NPTS,), 1.0, 6.0, ((0, 128),), jnp.float32),
        "len_low": draw_len_low(jax.random.fold_in(splits[10], 71), 0),
        "len_high": draw_len_high(jax.random.fold_in(splits[10], 71), 0),
        "variances": jnp.clip(jnp.exp(jax.random.uniform(splits[7], (2,), jnp.float32, math.log(0.5), math.log(2.0))), 0.5, 2.0),
        "nugget": jnp.clip(jnp.exp(jax.random.uniform(splits[8], (2,), jnp.float32, math.log(0.3), math.log(1.5))), 0.3, 1.5),
        "coupling": jnp.clip(jax.random.uniform(splits[9], (1,), jnp.float32, 0.6, 1.6), 0.6, 1.6),
    }


def point_factors(labels, coupling, nugget):
    fidelity = jnp.repeat(labels, 128).astype(jnp.float32)
    row_scale = 1.0 + (coupling[0] - 1.0) * fidelity
    nugget_points = nugget[0] + (nugget[1] - nugget[0]) * fidelity
    return row_scale, fidelity, nugget_points


def reference(points, labels, solution, residual, direction, len_low, len_high, variances, nugget, coupling):
    row_scale, high_mask, nugget_points = point_factors(labels, coupling, nugget)
    low_coords = points / len_low[:, None]
    high_coords = points / len_high[:, None]
    low_norms = jnp.sum(low_coords * low_coords, 0)
    high_norms = jnp.sum(high_coords * high_coords, 0)
    weights_low = row_scale * direction
    weights_high = high_mask * direction
    point_count = points.shape[1]
    row_block = 1024
    numbers = (point_count // row_block)
    dims = (((0,), (0,)), ((), ()))

    def block_rows(block_index):
        offset = block_index * row_block
        block_low = lax.dynamic_slice_in_dim(low_coords, offset, row_block, 1)
        block_high = lax.dynamic_slice_in_dim(high_coords, offset, row_block, 1)
        norm_low = lax.dynamic_slice_in_dim(low_norms, offset, row_block, 0)
        norm_high = lax.dynamic_slice_in_dim(high_norms, offset, row_block, 0)
        dist_low = norm_low[:, None] + low_norms[None, :] - 2.0 * lax.dot_general(
            block_low, low_coords, dims, precision=lax.Precision.HIGHEST)
        dist_high = norm_high[:, None] + high_norms[None, :] - 2.0 * lax.dot_general(
            block_high, high_coords, dims, precision=lax.Precision.HIGHEST)
        sum_low = jnp.dot(jnp.exp(-0.5 * dist_low), weights_low, precision=lax.Precision.HIGHEST)
        sum_high = jnp.dot(jnp.exp(-0.5 * dist_high), weights_high, precision=lax.Precision.HIGHEST)
        return sum_low, sum_high

    sum_low, sum_high = lax.map(block_rows, jnp.arange(numbers, dtype=jnp.int32))
    sum_low = sum_low.reshape(-1)
    sum_high = sum_high.reshape(-1)
    kernel_image = variances[0] * row_scale * sum_low + variances[1] * high_mask * sum_high + nugget_points * direction
    old_norm = jnp.sum(residual * residual)
    curvature = jnp.sum(direction * kernel_image)
    step_size = old_norm / curvature
    solution_next = solution + step_size * direction
    residual_next = residual - step_size * kernel_image
    new_norm = jnp.sum(residual_next * residual_next)
    direction_next = residual_next + (new_norm / old_norm) * direction
    return solution_next, residual_next, direction_next
```

```python
import functools
import itertools
import math

import jax
import jax.numpy as jnp
from jax import lax
from jax.experimental import pallas as pl
from jax.experimental.pallas import tpu as pltpu
from jax.sharding import PartitionSpec as P

MESH = pl.DeviceIdType.MESH
F32 = jnp.float32
BF16 = jnp.bfloat16
LOG2E = math.log2(math.e)
MASKED = -2000.0
WIDTH = 256
ROWS = 72

OFFSETS = [
    (0, 0, 0, 0),
    (1, 0, 0, 0),
    (0, 0, -1, 0),
    (0, 1, 0, 1),
    (-1, 0, 0, 1),
    (0, -1, -1, 1),
    (0, 1, 1, 0),
    (-1, 0, -1, 1),
    (-1, 1, 0, 1),
    (1, -1, 1, 0),
    (1, -1, 1, 1),
    (-1, -1, -1, 1),
    (-1, -1, 1, 0),
    (1, 1, -1, 1),
    (1, 1, 1, 1),
]
SOURCE = {s: (OFFSETS[s], 0) for s in range(1, len(OFFSETS))}
SEND_ORDER = [14, 13, 12, 11, 10, 9, 8, 7, 6, 5, 4, 3, 2, 1]
ARRIVAL = [0, 14, 13, 12, 11, 10, 9, 8, 7, 6, 5, 4, 3, 2, 1]


def diff(a, b):
    return ((a[0] - b[0]) % 4, (a[1] - b[1]) % 4, (a[2] - b[2]) % 4, (a[3] - b[3]) % 2)


def plan_units():
    rank = {s: i for i, s in enumerate(ARRIVAL)}
    seen, units = {(0, 0, 0, 0)}, {i: [] for i in range(len(OFFSETS))}
    units[0].append((0, 0, False))
    pairs = sorted(itertools.combinations(range(len(OFFSETS)), 2), key=lambda p: max(rank[p[0]], rank[p[1]]))
    for p in pairs:
        a, b = sorted(p, key=lambda s: rank[s])
        d, e = diff(OFFSETS[b], OFFSETS[a]), diff(OFFSETS[a], OFFSETS[b])
        if d in seen:
            continue
        seen.update((d, e))
        units[rank[b]].append((a, b, d != e))
    assert len(seen) == 128
    return units


UNITS = plan_units()


def place():
    r, c = lax.axis_index("row"), lax.axis_index("col")
    return c % 4, r // 4, (c // 4) * 2 + (r // 2) % 2, r % 2


def device_at(x, y, z, k):
    return ((y * 2 + z % 2) * 2 + k, (z // 2) * 4 + x)


def moved(me, offset, sign):
    x, y, z, k = me
    return device_at(
        (x + sign * offset[0] + 4) % 4,
        (y + sign * offset[1] + 4) % 4,
        (z + sign * offset[2] + 4) % 4,
        (k + offset[3]) % 2,
    )


def column_of(row, lanes):
    return jnp.broadcast_to(row, (lanes, row.shape[1])).T


def kernel(
    points_ref,
    labels_ref,
    solution_ref,
    residual_ref,
    direction_ref,
    len_low_ref,
    len_high_ref,
    variances_ref,
    nugget_ref,
    coupling_ref,
    sol_out,
    res_out,
    dir_out,
    raw,
    lhs,
    rhs,
    dir_col,
    dir_row,
    acc_col,
    acc_row,
    part,
    back,
    sums_a,
    sums_b,
    load_sem,
    send_sem,
    recv_sem,
    back_send,
    back_recv,
    a_send,
    a_recv,
    b_send,
    b_recv,
):
    n = len(OFFSETS)
    me = place()
    x, y, z, k = me
    load = pltpu.make_async_copy(points_ref, raw.at[0, pl.ds(0, 64)], load_sem)
    load.start()

    group_a = [(i, zb, kk) for i in range(4) for zb in range(2) for kk in range(2)]
    group_b = [(i, zb) for i in range(4) for zb in range(2)]
    peers_a = []
    for i, zb, kk in group_a[1:]:
        peers_a.append(device_at((x + i) % 4, y, (z // 2) * 2 + (z + zb) % 2, (k + kk) % 2))
    peers_b = []
    for i, zb in group_b[1:]:
        zz = 3 - z if zb else z
        peers_b.append(device_at(x, (y + i) % 4, zz, k))

    targets = [moved(me, SOURCE[s][0], -1) for s in range(1, n)]
    owners = [moved(me, OFFSETS[s], 1) for s in range(1, n)]

    barrier = pltpu.get_barrier_semaphore()
    greet = targets + owners + peers_a + peers_b
    for d in greet:
        pl.semaphore_signal(barrier, inc=1, device_id=d, device_id_type=MESH)

    lane = lax.broadcasted_iota(jnp.int32, (1, WIDTH), 1)
    first, second = labels_ref[0].astype(F32), labels_ref[1].astype(F32)
    label = jnp.where(lane < 128, first, second)
    direction = direction_ref[...]
    sub = lax.broadcasted_iota(jnp.int32, (8, WIDTH), 0)
    raw[0, pl.ds(64, 8), :] = jnp.where(sub == 0, direction, jnp.where(sub == 1, label, 0.0))

    root = math.sqrt(LOG2E)
    scales = [
        root / column_of(len_low_ref[...], 128),
        root / column_of(len_high_ref[...], 128),
    ]
    ones = jnp.ones((1, 128), F32)
    log_var = [0.5 * LOG2E * jnp.log(ones * variances_ref[0]), 0.5 * LOG2E * jnp.log(ones * variances_ref[1])]
    log_scale = LOG2E * jnp.log(ones * coupling_ref[0])
    wide = lambda v: jnp.concatenate([v, v], axis=1)
    log_var = [wide(v) for v in log_var]
    log_scale = wide(log_scale)

    load.wait()
    pl.semaphore_wait(barrier, len(greet))

    def copy_to(s):
        return pltpu.make_async_remote_copy(
            src_ref=raw.at[SOURCE[s][1]],
            dst_ref=raw.at[s],
            send_sem=send_sem.at[s],
            recv_sem=recv_sem.at[s],
            device_id=targets[s - 1],
            device_id_type=MESH,
        )

    for s in SEND_ORDER:
        if SOURCE[s][1] == 0:
            copy_to(s).start()

    acc_col[...] = jnp.zeros_like(acc_col)
    acc_row[...] = jnp.zeros_like(acc_row)

    row16 = lax.broadcasted_iota(jnp.int32, (16, WIDTH), 0)
    zeros48 = jnp.zeros((48, WIDTH), BF16)

    def prepare(s, as_lhs, as_rhs):
        pts = raw[s, pl.ds(0, 64), :]
        d = raw[s, pl.ds(64, 1), :]
        lab = raw[s, pl.ds(65, 1), :]
        for which in range(2):
            zz = pts * wide(scales[which])
            hi = zz.astype(BF16)
            hif = hi.astype(F32)
            lo = (zz - hif).astype(BF16)
            norm = jnp.sum(hif * (hif + 2.0 * lo.astype(F32)), axis=0, keepdims=True)
            extra = lab * log_scale if which == 0 else (1.0 - lab) * MASKED
            g = log_var[which] + extra - 0.5 * norm
            g1 = g.astype(BF16).astype(F32)
            g2 = (g - g1).astype(BF16).astype(F32)
            g3 = g - g1 - g2
            if as_lhs:
                e = jnp.where(row16 == 0, g1, jnp.where(row16 == 1, g2, jnp.where(row16 == 2, g3, 0.0)))
                e = jnp.where((row16 >= 3) & (row16 < 6), 1.0, e)
                full = jnp.concatenate([hi, hi, lo, e.astype(BF16), zeros48], axis=0)
                lhs[which, s] = full.T
            if as_rhs:
                e = jnp.where(row16 == 3, g1, jnp.where(row16 == 4, g2, jnp.where(row16 == 5, g3, 0.0)))
                e = jnp.where(row16 < 3, 1.0, e)
                rhs[which, s] = jnp.concatenate([hi, lo, hi, e.astype(BF16), zeros48], axis=0)
        dir_row[s] = jnp.broadcast_to(d, (8, WIDTH))
        if as_lhs:
            dir_col[s] = column_of(d, 128)

    def unit(a, b, both):
        el = jnp.dot(lhs[0, a], rhs[0, b], preferred_element_type=F32)
        eh = jnp.dot(lhs[1, a], rhs[1, b], preferred_element_type=F32)
        m = (jnp.exp2(el) + jnp.exp2(eh)).reshape(WIDTH // 8, 8, WIDTH)
        d = dir_col[a].reshape(WIDTH // 8, 8, 128)
        acc_col[b] += jnp.sum(m * jnp.concatenate([d, d], axis=2), axis=0)
        if both:
            t = m * dir_row[b][None]
            t = t[:, :, :128] + t[:, :, 128:]
            acc_row[a] += t.reshape(WIDTH, 128)

    flat = [u for us in UNITS.values() for u in us]
    is_lhs = {a for a, _, _ in flat}
    is_rhs = {b for _, b, _ in flat}
    has_row = {a for a, _, both in flat if both}
    for i, s in enumerate(ARRIVAL):
        if s > 0:
            copy_to(s).wait_recv()
        prepare(s, s in is_lhs, s in is_rhs)
        for u in UNITS[i]:
            unit(*u)

    def total_of(s):
        t = jnp.zeros((1, WIDTH), F32)
        if s in is_rhs:
            t = t + jnp.sum(acc_col[s], axis=0, keepdims=True)
        if s in has_row:
            t = t + jnp.sum(acc_row[s].T, axis=0, keepdims=True)
        return t

    def hand_back(s):
        return pltpu.make_async_remote_copy(
            src_ref=part.at[s],
            dst_ref=back.at[s],
            send_sem=back_send.at[s],
            recv_sem=back_recv.at[s],
            device_id=owners[s - 1],
            device_id_type=MESH,
        )

    for s in range(1, n):
        part[s] = total_of(s)
    for s in range(1, n):
        hand_back(s).start()
    image = total_of(0)
    nugget_points = nugget_ref[0] + (nugget_ref[1] - nugget_ref[0]) * label
    image = image + nugget_points * direction
    residual = residual_ref[...]
    for s in range(1, n):
        hand_back(s).wait_recv()
        image = image + back[s]

    def fold(v):
        return v[:, :128] + v[:, 128:]

    mine = jnp.concatenate(
        [
            fold(residual * residual),
            fold(direction * image),
            fold(residual * image),
            fold(image * image),
            jnp.zeros((4, 128), F32),
        ],
        axis=0,
    )

    sums_a[0] = mine

    def send_a(i):
        return pltpu.make_async_remote_copy(
            src_ref=sums_a.at[0],
            dst_ref=sums_a.at[i],
            send_sem=a_send.at[i],
            recv_sem=a_recv.at[i],
            device_id=peers_a[i - 1],
            device_id_type=MESH,
        )

    for i in range(1, 16):
        send_a(i).start()
    total = mine
    for i in range(1, 16):
        send_a(i).wait_recv()
        total = total + sums_a[i]
    sums_b[0] = total

    def send_b(i):
        return pltpu.make_async_remote_copy(
            src_ref=sums_b.at[0],
            dst_ref=sums_b.at[i],
            send_sem=b_send.at[i],
            recv_sem=b_recv.at[i],
            device_id=peers_b[i - 1],
            device_id_type=MESH,
        )

    for i in range(1, 8):
        send_b(i).start()
    for i in range(1, 8):
        send_b(i).wait_recv()
        total = total + sums_b[i]

    scal = jnp.sum(total, axis=1, keepdims=True)
    old_norm, curvature, cross, image_norm = scal[0:1], scal[1:2], scal[2:3], scal[3:4]
    step = old_norm / curvature
    new_norm = old_norm - 2.0 * step * cross + step * step * image_norm
    sol_out[...] = solution_ref[...] + step * direction
    res_next = residual - step * image
    res_out[...] = res_next
    dir_out[...] = res_next + new_norm / old_norm * direction

    for s in range(1, n):
        copy_to(s).wait_send()
        hand_back(s).wait_send()
    for i in range(1, 16):
        send_a(i).wait_send()
    for i in range(1, 8):
        send_b(i).wait_send()


def body(points, labels, solution, residual, direction, len_low, len_high, variances, nugget, coupling):
    n = len(OFFSETS)
    vmem = pl.BlockSpec(memory_space=pltpu.VMEM)
    smem = pl.BlockSpec(memory_space=pltpu.SMEM)
    row = lambda v: v.reshape(1, v.shape[0])
    outs = pl.pallas_call(
        kernel,
        out_shape=[jax.ShapeDtypeStruct((1, WIDTH), F32)] * 3,
        in_specs=[pl.BlockSpec(memory_space=pl.ANY), smem, vmem, vmem, vmem, vmem, vmem, smem, smem, smem],
        out_specs=[vmem] * 3,
        scratch_shapes=[
            pltpu.VMEM((n, ROWS, WIDTH), F32),
            pltpu.VMEM((2, n, WIDTH, WIDTH), BF16),
            pltpu.VMEM((2, n, WIDTH, WIDTH), BF16),
            pltpu.VMEM((n, WIDTH, 128), F32),
            pltpu.VMEM((n, 8, WIDTH), F32),
            pltpu.VMEM((n, 8, WIDTH), F32),
            pltpu.VMEM((n, WIDTH, 128), F32),
            pltpu.VMEM((n, 1, WIDTH), F32),
            pltpu.VMEM((n, 1, WIDTH), F32),
            pltpu.VMEM((16, 8, 128), F32),
            pltpu.VMEM((8, 8, 128), F32),
            pltpu.SemaphoreType.DMA,
            pltpu.SemaphoreType.DMA((n,)),
            pltpu.SemaphoreType.DMA((n,)),
            pltpu.SemaphoreType.DMA((n,)),
            pltpu.SemaphoreType.DMA((n,)),
            pltpu.SemaphoreType.DMA((16,)),
            pltpu.SemaphoreType.DMA((16,)),
            pltpu.SemaphoreType.DMA((8,)),
            pltpu.SemaphoreType.DMA((8,)),
        ],
        compiler_params=pltpu.CompilerParams(
            collective_id=0, has_side_effects=True, vmem_limit_bytes=56 * 2**20
        ),
    )(
        points,
        labels,
        row(solution),
        row(residual),
        row(direction),
        row(len_low),
        row(len_high),
        variances,
        nugget,
        coupling,
    )
    return tuple(o.reshape(WIDTH) for o in outs)


def solution(mesh):
    both = P(("row", "col"))
    in_specs = (P(None, ("row", "col")), both, both, both, both, P(), P(), P(), P(), P())
    return jax.shard_map(body, mesh=mesh, in_specs=in_specs, out_specs=(both, both, both), check_vma=False)
```

```python
import functools
import itertools
import math

import jax
import jax.numpy as jnp
from jax import lax
from jax.experimental import pallas as pl
from jax.experimental.pallas import tpu as pltpu
from jax.sharding import PartitionSpec as P

MESH = pl.DeviceIdType.MESH
F32 = jnp.float32
BF16 = jnp.bfloat16
LOG2E = math.log2(math.e)
MASKED = -2000.0
WIDTH = 256
ROWS = 72

PLAN = [
    ((0, 0, 0, 0), (0, 0, 0, 0)),
    ((0, 0, 0, 1), (0, 0, 0, 1)),
    ((0, 1, 0, 0), (0, 1, 0, 0)),
    ((-1, -1, 0, 0), (-1, -1, 0, 0)),
    ((-1, 0, -1, 0), (-1, 0, -1, 0)),
    ((1, 0, -1, 0), (1, 0, -1, 0)),
    ((1, 0, 1, 0), (1, 0, 1, 0)),
    ((-1, 0, -1, 1), (0, 0, 0, 1)),
    ((0, 2, 0, 0), (0, 1, 0, 0)),
    ((1, 0, -1, 1), (0, 0, 0, 1)),
    ((1, 1, 0, 0), (1, 0, 0, 0)),
    ((-1, 0, 2, 1), (0, 0, -1, 1)),
    ((-1, 2, 0, 0), (0, -1, 0, 0)),
    ((1, 0, 2, 0), (0, 0, 1, 0)),
    ((2, -1, 0, 1), (-1, 0, 0, 1)),
    ((-1, 2, 0, 1), (0, 0, 0, 1)),
]
OFFSETS = [row[0] for row in PLAN]


def diff(a, b):
    return ((a[0] - b[0]) % 4, (a[1] - b[1]) % 4, (a[2] - b[2]) % 4, (a[3] - b[3]) % 2)


HELD = [diff(block, (0, 0, 0, 0)) for block, _ in PLAN]
ORIGIN = [HELD.index(diff(block, sender)) for block, sender in PLAN]


def plan_units():
    seen, units = {(0, 0, 0, 0)}, [[] for _ in OFFSETS]
    units[0].append((0, 0, False))
    for a, b in sorted(itertools.combinations(range(len(OFFSETS)), 2), key=lambda p: p[1]):
        d, e = diff(OFFSETS[b], OFFSETS[a]), diff(OFFSETS[a], OFFSETS[b])
        if d in seen:
            continue
        seen.update((d, e))
        units[b].append((a, b, d != e))
    assert len(seen) == 128
    return units


UNITS = plan_units()


def place():
    r, c = lax.axis_index("row"), lax.axis_index("col")
    return c % 4, r // 4, (c // 4) * 2 + (r // 2) % 2, r % 2


def device_at(x, y, z, k):
    return ((y * 2 + z % 2) * 2 + k, (z // 2) * 4 + x)


def moved(me, offset, sign):
    x, y, z, k = me
    return device_at(
        (x + sign * offset[0] + 4) % 4,
        (y + sign * offset[1] + 4) % 4,
        (z + sign * offset[2] + 4) % 4,
        (k + offset[3]) % 2,
    )


def column_of(row, lanes):
    return jnp.broadcast_to(row, (lanes, row.shape[1])).T


def kernel(
    points_in,
    labels_in,
    solution_in,
    residual_in,
    direction_in,
    len_low_in,
    len_high_in,
    variances_in,
    nugget_in,
    coupling_in,
    out_ref,
    raw,
    aux,
    lhs,
    rhs,
    dir_col,
    dir_row,
    acc_col,
    acc_row,
    part,
    back,
    sums_a,
    sums_b,
    labels_ref,
    solution_ref,
    residual_ref,
    direction_ref,
    len_low_ref,
    len_high_ref,
    variances_ref,
    nugget_ref,
    coupling_ref,
    load_sem,
    send_sem,
    recv_sem,
    aux_send,
    aux_recv,
    back_send,
    back_recv,
    a_send,
    a_recv,
    b_send,
    b_recv,
):
    n = len(OFFSETS)
    me = place()
    x, y, z, k = me
    group_a = [(i, zb, kk) for i in range(4) for zb in range(2) for kk in range(2)]
    group_b = [(i, zb) for i in range(4) for zb in range(2)]
    peers_a = []
    for i, zb, kk in group_a[1:]:
        peers_a.append(device_at((x + i) % 4, y, (z // 2) * 2 + (z + zb) % 2, (k + kk) % 2))
    peers_b = []
    for i, zb in group_b[1:]:
        zz = 3 - z if zb else z
        peers_b.append(device_at(x, (y + i) % 4, zz, k))

    targets = [moved(me, PLAN[s][1], -1) for s in range(1, n)]
    owners = [moved(me, OFFSETS[s], 1) for s in range(1, n)]

    barrier = pltpu.get_barrier_semaphore()
    near = sorted({row[1] for row in PLAN[1:]})
    greet = [moved(me, f, -1) for f in near] + [moved(me, f, 1) for f in near if diff(f, (0, 0, 0, 0)) != diff((0, 0, 0, 0), f)]
    for d in greet:
        pl.semaphore_signal(barrier, inc=1, device_id=d, device_id_type=MESH)

    pairs = [
        (labels_in, labels_ref),
        (direction_in, direction_ref),
        (points_in, raw.at[0]),
        (len_low_in, len_low_ref),
        (len_high_in, len_high_ref),
        (coupling_in, coupling_ref),
        (variances_in, variances_ref),
        (nugget_in, nugget_ref),
        (residual_in, residual_ref),
        (solution_in, solution_ref),
    ]
    loads = [pltpu.make_async_copy(src, dst, load_sem.at[i]) for i, (src, dst) in enumerate(pairs)]
    for load in loads:
        load.start()
    for load in loads[:2]:
        load.wait()
    lane = lax.broadcasted_iota(jnp.int32, (1, WIDTH), 1)
    fidelity = labels_ref[...].astype(F32)
    label = jnp.where(lane < 128, fidelity[:, 0:1], fidelity[:, 1:2])
    direction = direction_ref[...]
    aux[0] = jnp.concatenate([direction, label], axis=1)
    loads[2].wait()
    pl.semaphore_wait(barrier, len(greet))

    def copy_to(s):
        return pltpu.make_async_remote_copy(
            src_ref=raw.at[ORIGIN[s]],
            dst_ref=raw.at[s],
            send_sem=send_sem.at[s],
            recv_sem=recv_sem.at[s],
            device_id=targets[s - 1],
            device_id_type=MESH,
        )

    def aux_to(s):
        return pltpu.make_async_remote_copy(
            src_ref=aux.at[ORIGIN[s]],
            dst_ref=aux.at[s],
            send_sem=aux_send.at[s],
            recv_sem=aux_recv.at[s],
            device_id=targets[s - 1],
            device_id_type=MESH,
        )

    def pass_on(q):
        for s in range(1, n):
            if ORIGIN[s] == q:
                copy_to(s).start()
                aux_to(s).start()

    pass_on(0)
    for load in loads[3:]:
        load.wait()

    root = math.sqrt(LOG2E)
    scales = [
        root / column_of(len_low_ref[...], 128),
        root / column_of(len_high_ref[...], 128),
    ]
    ones = jnp.ones((1, 128), F32)
    log_var = [0.5 * LOG2E * jnp.log(ones * variances_ref[0:1, 0:1]), 0.5 * LOG2E * jnp.log(ones * variances_ref[0:1, 1:2])]
    log_scale = LOG2E * jnp.log(ones * coupling_ref[0:1, 0:1])
    wide = lambda v: jnp.concatenate([v, v], axis=1)
    log_var = [wide(v) for v in log_var]
    log_scale = wide(log_scale)

    acc_col[...] = jnp.zeros_like(acc_col)
    acc_row[...] = jnp.zeros_like(acc_row)

    row16 = lax.broadcasted_iota(jnp.int32, (16, WIDTH), 0)
    zeros48 = jnp.zeros((48, WIDTH), BF16)

    def prepare(s, as_lhs, as_rhs):
        pts = raw[s]
        d = aux[s][:, :WIDTH]
        lab = aux[s][:, WIDTH:]
        for which in range(2):
            zz = pts * wide(scales[which])
            hi = zz.astype(BF16)
            hif = hi.astype(F32)
            lo = (zz - hif).astype(BF16)
            norm = jnp.sum(hif * (hif + 2.0 * lo.astype(F32)), axis=0, keepdims=True)
            extra = lab * log_scale if which == 0 else (1.0 - lab) * MASKED
            g = log_var[which] + extra - 0.5 * norm
            g1 = g.astype(BF16).astype(F32)
            g2 = (g - g1).astype(BF16).astype(F32)
            g3 = g - g1 - g2
            if as_lhs:
                e = jnp.where(row16 == 0, g1, jnp.where(row16 == 1, g2, jnp.where(row16 == 2, g3, 0.0)))
                e = jnp.where((row16 >= 3) & (row16 < 6), 1.0, e)
                full = jnp.concatenate([hi, hi, lo, e.astype(BF16), zeros48], axis=0)
                lhs[which, s] = full.T
            if as_rhs:
                e = jnp.where(row16 == 3, g1, jnp.where(row16 == 4, g2, jnp.where(row16 == 5, g3, 0.0)))
                e = jnp.where(row16 < 3, 1.0, e)
                rhs[which, s] = jnp.concatenate([hi, lo, hi, e.astype(BF16), zeros48], axis=0)
        dir_row[s] = jnp.broadcast_to(d, (8, WIDTH))
        if as_lhs:
            dir_col[s] = column_of(d, 128)

    def unit(a, b, both):
        el = jnp.dot(lhs[0, a], rhs[0, b], preferred_element_type=F32)
        eh = jnp.dot(lhs[1, a], rhs[1, b], preferred_element_type=F32)
        m = (jnp.exp2(el) + jnp.exp2(eh)).reshape(WIDTH // 8, 8, WIDTH)
        d = dir_col[a].reshape(WIDTH // 8, 8, 128)
        acc_col[b] += jnp.sum(m * jnp.concatenate([d, d], axis=2), axis=0)
        if both:
            t = m * dir_row[b][None]
            t = t[:, :, :128] + t[:, :, 128:]
            acc_row[a] += t.reshape(WIDTH, 128)

    flat = [u for us in UNITS for u in us]
    is_lhs = {a for a, _, _ in flat}
    is_rhs = {b for _, b, _ in flat}
    has_row = {a for a, _, both in flat if both}
    for s in range(n):
        if s > 0:
            copy_to(s).wait_recv()
            aux_to(s).wait_recv()
            pass_on(s)
        prepare(s, s in is_lhs, s in is_rhs)
        for u in UNITS[s]:
            unit(*u)

    def total_of(s):
        t = jnp.zeros((1, WIDTH), F32)
        if s in is_rhs:
            t = t + jnp.sum(acc_col[s], axis=0, keepdims=True)
        if s in has_row:
            t = t + jnp.sum(acc_row[s].T, axis=0, keepdims=True)
        return t

    def hand_back(s):
        return pltpu.make_async_remote_copy(
            src_ref=part.at[s],
            dst_ref=back.at[s],
            send_sem=back_send.at[s],
            recv_sem=back_recv.at[s],
            device_id=owners[s - 1],
            device_id_type=MESH,
        )

    for s in range(1, n):
        part[s] = total_of(s)
        if s > 1:
            hand_back(s - 1).start()
    image = total_of(0)
    hand_back(n - 1).start()
    nugget_points = nugget_ref[0:1, 0:1] + (nugget_ref[0:1, 1:2] - nugget_ref[0:1, 0:1]) * label
    image = image + nugget_points * direction
    residual = residual_ref[...]
    for s in range(1, n):
        hand_back(s).wait_recv()
        image = image + back[s]

    def fold(v):
        return v[:, :128] + v[:, 128:]

    mine = jnp.concatenate(
        [
            fold(residual * residual),
            fold(direction * image),
            fold(residual * image),
            fold(image * image),
            jnp.zeros((4, 128), F32),
        ],
        axis=0,
    )

    sums_a[0] = mine

    def send_a(i):
        return pltpu.make_async_remote_copy(
            src_ref=sums_a.at[0],
            dst_ref=sums_a.at[i],
            send_sem=a_send.at[i],
            recv_sem=a_recv.at[i],
            device_id=peers_a[i - 1],
            device_id_type=MESH,
        )

    for i in range(1, 16):
        send_a(i).start()
    total = mine
    for i in range(1, 16):
        send_a(i).wait_recv()
        total = total + sums_a[i]
    sums_b[0] = total

    def send_b(i):
        return pltpu.make_async_remote_copy(
            src_ref=sums_b.at[0],
            dst_ref=sums_b.at[i],
            send_sem=b_send.at[i],
            recv_sem=b_recv.at[i],
            device_id=peers_b[i - 1],
            device_id_type=MESH,
        )

    for i in range(1, 8):
        send_b(i).start()
    for i in range(1, 8):
        send_b(i).wait_recv()
        total = total + sums_b[i]

    scal = jnp.sum(total, axis=1, keepdims=True)
    old_norm, curvature, cross, image_norm = scal[0:1], scal[1:2], scal[2:3], scal[3:4]
    step = old_norm / curvature
    new_norm = old_norm - 2.0 * step * cross + step * step * image_norm
    residual_next = residual - step * image
    out_ref[...] = jnp.concatenate(
        [
            solution_ref[...] + step * direction,
            residual_next,
            residual_next + new_norm / old_norm * direction,
        ],
        axis=0,
    )

    for s in range(1, n):
        copy_to(s).wait_send()
        aux_to(s).wait_send()
        hand_back(s).wait_send()
    for i in range(1, 16):
        send_a(i).wait_send()
    for i in range(1, 8):
        send_b(i).wait_send()


def body(points, labels, solution, residual, direction, len_low, len_high, variances, nugget, coupling):
    n = len(OFFSETS)
    row = lambda v: v.reshape(1, v.shape[0])
    taken = [
        points,
        row(labels),
        row(solution),
        row(residual),
        row(direction),
        row(len_low),
        row(len_high),
        row(variances),
        row(nugget),
        row(coupling),
    ]
    small = taken[1:]
    out = pl.pallas_call(
        kernel,
        out_shape=jax.ShapeDtypeStruct((3, WIDTH), F32),
        in_specs=[pl.BlockSpec(memory_space=pl.ANY)] * len(taken),
        out_specs=pl.BlockSpec(memory_space=pltpu.VMEM),
        scratch_shapes=[
            pltpu.VMEM((n, 64, WIDTH), F32),
            pltpu.VMEM((n, 1, 2 * WIDTH), F32),
            pltpu.VMEM((2, n, WIDTH, WIDTH), BF16),
            pltpu.VMEM((2, n, WIDTH, WIDTH), BF16),
            pltpu.VMEM((n, WIDTH, 128), F32),
            pltpu.VMEM((n, 8, WIDTH), F32),
            pltpu.VMEM((n, 8, WIDTH), F32),
            pltpu.VMEM((n, WIDTH, 128), F32),
            pltpu.VMEM((n, 1, WIDTH), F32),
            pltpu.VMEM((n, 1, WIDTH), F32),
            pltpu.VMEM((16, 8, 128), F32),
            pltpu.VMEM((8, 8, 128), F32),
            *[pltpu.VMEM(v.shape, v.dtype) for v in small],
            pltpu.SemaphoreType.DMA((len(taken),)),
            *[pltpu.SemaphoreType.DMA((n,)) for _ in range(6)],
            pltpu.SemaphoreType.DMA((16,)),
            pltpu.SemaphoreType.DMA((16,)),
            pltpu.SemaphoreType.DMA((8,)),
            pltpu.SemaphoreType.DMA((8,)),
        ],
        compiler_params=pltpu.CompilerParams(
            collective_id=0, has_side_effects=True, vmem_limit_bytes=56 * 2**20
        ),
    )(*taken)
    return out[0], out[1], out[2]


def solution(mesh):
    both = P(("row", "col"))
    in_specs = (P(None, ("row", "col")), both, both, both, both, P(), P(), P(), P(), P())
    return jax.shard_map(body, mesh=mesh, in_specs=in_specs, out_specs=(both, both, both), check_vma=False)
```

```python
import functools
import itertools
import math

import jax
import jax.numpy as jnp
from jax import lax
from jax.experimental import pallas as pl
from jax.experimental.pallas import tpu as pltpu
from jax.sharding import PartitionSpec as P

MESH = pl.DeviceIdType.MESH
F32 = jnp.float32
BF16 = jnp.bfloat16
LOG2E = math.log2(math.e)
MASKED = -2000.0
WIDTH = 256
PARTS = 1
SHIFTS = (2, 1, 3, 0)

PLAN = [
    ((0, 0, 0, 0), (0, 0, 0, 0)),
    ((0, 0, 0, 1), (0, 0, 0, 1)),
    ((0, 1, 0, 0), (0, 1, 0, 0)),
    ((-1, -1, 0, 0), (-1, -1, 0, 0)),
    ((-1, 0, -1, 0), (-1, 0, -1, 0)),
    ((1, 0, -1, 0), (1, 0, -1, 0)),
    ((1, 0, 1, 0), (1, 0, 1, 0)),
    ((-1, 0, -1, 1), (0, 0, 0, 1)),
    ((0, 2, 0, 0), (0, 1, 0, 0)),
    ((1, 0, -1, 1), (0, 0, 0, 1)),
    ((1, 1, 0, 0), (1, 0, 0, 0)),
    ((-1, 0, 2, 1), (0, 0, -1, 1)),
    ((-1, 2, 0, 0), (0, -1, 0, 0)),
    ((1, 0, 2, 0), (0, 0, 1, 0)),
    ((2, -1, 0, 1), (-1, 0, 0, 1)),
    ((-1, 2, 0, 1), (0, 0, 0, 1)),
]
OFFSETS = [row[0] for row in PLAN]


def diff(a, b):
    return ((a[0] - b[0]) % 4, (a[1] - b[1]) % 4, (a[2] - b[2]) % 4, (a[3] - b[3]) % 2)


HELD = [diff(block, (0, 0, 0, 0)) for block, _ in PLAN]
ORIGIN = [HELD.index(diff(block, sender)) for block, sender in PLAN]


def plan_units():
    seen, units = {(0, 0, 0, 0)}, [[] for _ in OFFSETS]
    units[0].append((0, 0, False))
    for a, b in sorted(itertools.combinations(range(len(OFFSETS)), 2), key=lambda p: p[1]):
        d, e = diff(OFFSETS[b], OFFSETS[a]), diff(OFFSETS[a], OFFSETS[b])
        if d in seen:
            continue
        seen.update((d, e))
        units[b].append((a, b, d != e))
    assert len(seen) == 128
    return units


UNITS = plan_units()
STEPS = [(range(1, 7), range(0, 4)), (range(7, 11), range(4, 8)), (range(11, 13), range(8, 11)), (range(13, 16), range(11, 16))]


def place():
    r, c = lax.axis_index("row"), lax.axis_index("col")
    return c % 4, r // 4, (c // 4) * 2 + (r // 2) % 2, r % 2


def device_at(x, y, z, k):
    return ((y * 2 + z % 2) * 2 + k, (z // 2) * 4 + x)


def moved(me, offset, sign):
    x, y, z, k = me
    return device_at(
        (x + sign * offset[0] + 8) % 4,
        (y + sign * offset[1] + 4) % 4,
        (z + sign * offset[2] + 4) % 4,
        (k + offset[3]) % 2,
    )


def column_of(row, lanes):
    return jnp.broadcast_to(row, (lanes, row.shape[1])).T


def kernel(
    points_in,
    labels_in,
    solution_in,
    residual_in,
    direction_in,
    len_low_in,
    len_high_in,
    variances_in,
    nugget_in,
    coupling_in,
    out_ref,
    raw,
    aux,
    lhs,
    rhs,
    dir_col,
    dir_row,
    acc_col,
    acc_row,
    part,
    back,
    own,
    sums,
    labels_ref,
    solution_ref,
    residual_ref,
    direction_ref,
    len_low_ref,
    len_high_ref,
    variances_ref,
    nugget_ref,
    coupling_ref,
    load_sem,
    send_sem,
    recv_sem,
    aux_send,
    aux_recv,
    back_send,
    back_recv,
    own_send,
    own_recv,
    sums_send,
    sums_recv,
):
    n = len(OFFSETS)
    me = place()
    x, y, z, k = me
    peers = []
    for j, l, kk in list(itertools.product(range(4), range(4), range(2)))[1:]:
        peers.append(device_at(x, (y + j) % 4, (z + l) % 4, (k + kk) % 2))

    targets = [moved(me, PLAN[s][1], -1) for s in range(1, n)]
    lines = [
        [moved(me, (dx + shift, dy, dz, dk), 1) for dx, dy, dz, dk in OFFSETS] for shift in range(4)
    ]

    barrier = pltpu.get_barrier_semaphore()
    near = sorted({row[1] for row in PLAN[1:]})
    greet = [moved(me, f, -1) for f in near] + [moved(me, f, 1) for f in near if diff(f, (0, 0, 0, 0)) != diff((0, 0, 0, 0), f)]
    for d in greet:
        pl.semaphore_signal(barrier, inc=1, device_id=d, device_id_type=MESH)

    pairs = [
        (labels_in, labels_ref),
        (direction_in, direction_ref),
        (points_in, raw.at[0]),
        (len_low_in, len_low_ref),
        (len_high_in, len_high_ref),
        (coupling_in, coupling_ref),
        (variances_in, variances_ref),
        (nugget_in, nugget_ref),
        (residual_in, residual_ref),
        (solution_in, solution_ref),
    ]
    loads = [pltpu.make_async_copy(src, dst, load_sem.at[i]) for i, (src, dst) in enumerate(pairs)]
    for load in loads:
        load.start()
    for load in loads[:2]:
        load.wait()
    lane = lax.broadcasted_iota(jnp.int32, (1, WIDTH), 1)
    fidelity = labels_ref[...].astype(F32)
    label = jnp.where(lane < 128, fidelity[:, 0:1], fidelity[:, 1:2])
    direction = direction_ref[...]
    aux[0] = jnp.concatenate([direction, label], axis=1)
    loads[2].wait()
    pl.semaphore_wait(barrier, len(greet))

    def copy_to(s, part_of):
        rows = pl.ds(part_of * (64 // PARTS), 64 // PARTS)
        return pltpu.make_async_remote_copy(
            src_ref=raw.at[ORIGIN[s], rows],
            dst_ref=raw.at[s, rows],
            send_sem=send_sem.at[s, part_of],
            recv_sem=recv_sem.at[s, part_of],
            device_id=targets[s - 1],
            device_id_type=MESH,
        )

    def aux_to(s):
        return pltpu.make_async_remote_copy(
            src_ref=aux.at[ORIGIN[s]],
            dst_ref=aux.at[s],
            send_sem=aux_send.at[s],
            recv_sem=aux_recv.at[s],
            device_id=targets[s - 1],
            device_id_type=MESH,
        )

    onward = [[s for s in range(1, n) if ORIGIN[s] == q] for q in range(n)]

    def pass_on(q, part_of):
        for s in onward[q]:
            copy_to(s, part_of).start()
            if part_of == 0:
                aux_to(s).start()

    def take(s):
        for part_of in range(PARTS):
            copy_to(s, part_of).wait_recv()
            if part_of == 0:
                aux_to(s).wait_recv()
            pass_on(s, part_of)

    for part_of in range(PARTS):
        pass_on(0, part_of)
    for load in loads[3:]:
        load.wait()

    root = math.sqrt(LOG2E)
    scales = [
        root / column_of(len_low_ref[...], 128),
        root / column_of(len_high_ref[...], 128),
    ]
    ones = jnp.ones((1, 128), F32)
    log_var = [0.5 * LOG2E * jnp.log(ones * variances_ref[0:1, 0:1]), 0.5 * LOG2E * jnp.log(ones * variances_ref[0:1, 1:2])]
    log_scale = LOG2E * jnp.log(ones * coupling_ref[...].reshape(1, 1))
    wide = lambda v: jnp.concatenate([v, v], axis=1)
    log_var = [wide(v) for v in log_var]
    log_scale = wide(log_scale)

    acc_col[...] = jnp.zeros_like(acc_col)
    acc_row[...] = jnp.zeros_like(acc_row)

    row16 = lax.broadcasted_iota(jnp.int32, (16, WIDTH), 0)
    zeros48 = jnp.zeros((48, WIDTH), BF16)

    def prepare(s, as_lhs, as_rhs):
        pts = raw[s]
        d = aux[s][:, :WIDTH]
        lab = aux[s][:, WIDTH:]
        for which in range(2):
            zz = pts * wide(scales[which])
            hi = zz.astype(BF16)
            hif = hi.astype(F32)
            lo = (zz - hif).astype(BF16)
            norm = jnp.sum(hif * (hif + 2.0 * lo.astype(F32)), axis=0, keepdims=True)
            extra = lab * log_scale if which == 0 else (1.0 - lab) * MASKED
            g = log_var[which] + extra - 0.5 * norm
            g1 = g.astype(BF16).astype(F32)
            g2 = (g - g1).astype(BF16).astype(F32)
            g3 = g - g1 - g2
            if as_lhs:
                e = jnp.where(row16 == 0, g1, jnp.where(row16 == 1, g2, jnp.where(row16 == 2, g3, 0.0)))
                e = jnp.where((row16 >= 3) & (row16 < 6), 1.0, e)
                full = jnp.concatenate([hi, hi, lo, e.astype(BF16), zeros48], axis=0)
                lhs[which, s] = full.T
            if as_rhs:
                e = jnp.where(row16 == 3, g1, jnp.where(row16 == 4, g2, jnp.where(row16 == 5, g3, 0.0)))
                e = jnp.where(row16 < 3, 1.0, e)
                rhs[which, s] = jnp.concatenate([hi, lo, hi, e.astype(BF16), zeros48], axis=0)
        dir_row[s] = jnp.broadcast_to(d, (8, WIDTH))
        if as_lhs:
            dir_col[s] = column_of(d, 128)

    def unit(a, b, both):
        el = jnp.dot(lhs[0, a], rhs[0, b], preferred_element_type=F32)
        eh = jnp.dot(lhs[1, a], rhs[1, b], preferred_element_type=F32)
        m = (jnp.exp2(el) + jnp.exp2(eh)).reshape(WIDTH // 8, 8, WIDTH)
        d = dir_col[a].reshape(WIDTH // 8, 8, 128)
        acc_col[b] += jnp.sum(m * jnp.concatenate([d, d], axis=2), axis=0)
        if both:
            t = m * dir_row[b][None]
            t = t[:, :, :128] + t[:, :, 128:]
            acc_row[a] += t.reshape(WIDTH, 128)

    flat = [u for us in UNITS for u in us]
    is_lhs = {a for a, _, _ in flat}
    is_rhs = {b for _, b, _ in flat}
    has_row = {a for a, _, both in flat if both}
    prepare(0, True, True)
    for taken, ready in STEPS:
        for s in taken:
            take(s)
        for s in taken:
            prepare(s, s in is_lhs, s in is_rhs)
        for u in sorted(u for s in ready for u in UNITS[s]):
            unit(*u)

    def total_of(s):
        t = jnp.zeros((1, WIDTH), F32)
        if s in is_rhs:
            t = t + jnp.sum(acc_col[s], axis=0, keepdims=True)
        if s in has_row:
            t = t + jnp.sum(acc_row[s].T, axis=0, keepdims=True)
        return t

    def hand_back(s, shift):
        return pltpu.make_async_remote_copy(
            src_ref=part.at[s],
            dst_ref=back.at[shift, s],
            send_sem=back_send.at[shift, s],
            recv_sem=back_recv.at[shift, s],
            device_id=lines[shift][s],
            device_id_type=MESH,
        )

    def hand_own(shift):
        return pltpu.make_async_remote_copy(
            src_ref=own.at[0],
            dst_ref=own.at[shift],
            send_sem=own_send.at[shift],
            recv_sem=own_recv.at[shift],
            device_id=lines[shift][0],
            device_id_type=MESH,
        )

    residual = residual_ref[...]
    nugget_points = nugget_ref[0:1, 0:1] + (nugget_ref[0:1, 1:2] - nugget_ref[0:1, 0:1]) * label
    order = list(range(n - 1, 0, -1))
    for at, s in enumerate(order):
        part[s] = total_of(s)
        if at > 0:
            for shift in SHIFTS:
                hand_back(order[at - 1], shift).start()
    image = total_of(0) + nugget_points * direction
    own[0] = jnp.concatenate([image, residual, direction], axis=1)
    for shift in SHIFTS:
        hand_back(order[-1], shift).start()
    for shift in SHIFTS[:-1]:
        hand_own(shift).start()

    def fold(v):
        return v[:, :128] + v[:, 128:]

    total = jnp.zeros((4, 128), F32)
    for shift in (0, 1, 3, 2):
        if shift > 0:
            hand_own(shift).wait_recv()
        y_line, r_line, d_line = (own[shift][:, at * WIDTH : (at + 1) * WIDTH] for at in range(3))
        for s in order:
            hand_back(s, shift).wait_recv()
            y_line = y_line + back[shift, s]
        if shift == 0:
            image = y_line
        total = total + jnp.concatenate(
            [fold(r_line * r_line), fold(d_line * y_line), fold(r_line * y_line), fold(y_line * y_line)],
            axis=0,
        )
    sums[0] = total

    def send_sums(i):
        return pltpu.make_async_remote_copy(
            src_ref=sums.at[0],
            dst_ref=sums.at[i],
            send_sem=sums_send.at[i],
            recv_sem=sums_recv.at[i],
            device_id=peers[i - 1],
            device_id_type=MESH,
        )

    for i in range(31, 0, -1):
        send_sums(i).start()
    for i in range(1, 32):
        send_sums(i).wait_recv()
        total = total + sums[i]

    scal = jnp.sum(total, axis=1, keepdims=True)
    old_norm, curvature, cross, image_norm = scal[0:1], scal[1:2], scal[2:3], scal[3:4]
    step = old_norm / curvature
    new_norm = old_norm - 2.0 * step * cross + step * step * image_norm
    residual_next = residual - step * image
    out_ref[...] = jnp.concatenate(
        [
            solution_ref[...] + step * direction,
            residual_next,
            residual_next + new_norm / old_norm * direction,
        ],
        axis=0,
    )

    for s in range(1, n):
        for part_of in range(PARTS):
            copy_to(s, part_of).wait_send()
        aux_to(s).wait_send()
        for shift in SHIFTS:
            hand_back(s, shift).wait_send()
    for shift in SHIFTS[:-1]:
        hand_own(shift).wait_send()
    for i in range(1, 32):
        send_sums(i).wait_send()


def body(points, labels, solution, residual, direction, len_low, len_high, variances, nugget, coupling):
    n = len(OFFSETS)
    row = lambda v: v.reshape(1, v.shape[0])
    taken = [
        points,
        row(labels),
        row(solution),
        row(residual),
        row(direction),
        row(len_low),
        row(len_high),
        row(variances),
        row(nugget),
        coupling,
    ]
    small = taken[1:]
    out = pl.pallas_call(
        kernel,
        out_shape=jax.ShapeDtypeStruct((3, WIDTH), F32),
        in_specs=[pl.BlockSpec(memory_space=pl.ANY)] * len(taken),
        out_specs=pl.BlockSpec(memory_space=pltpu.VMEM),
        scratch_shapes=[
            pltpu.VMEM((n, 64, WIDTH), F32),
            pltpu.VMEM((n, 1, 2 * WIDTH), F32),
            pltpu.VMEM((2, n, WIDTH, WIDTH), BF16),
            pltpu.VMEM((2, n, WIDTH, WIDTH), BF16),
            pltpu.VMEM((n, WIDTH, 128), F32),
            pltpu.VMEM((n, 8, WIDTH), F32),
            pltpu.VMEM((n, 8, WIDTH), F32),
            pltpu.VMEM((n, WIDTH, 128), F32),
            pltpu.VMEM((n, 1, WIDTH), F32),
            pltpu.VMEM((4, n, 1, WIDTH), F32),
            pltpu.VMEM((4, 1, 3 * WIDTH), F32),
            pltpu.VMEM((32, 4, 128), F32),
            *[pltpu.VMEM(v.shape, v.dtype) for v in small],
            pltpu.SemaphoreType.DMA((len(taken),)),
            *[pltpu.SemaphoreType.DMA((n, PARTS)) for _ in range(2)],
            *[pltpu.SemaphoreType.DMA((n,)) for _ in range(2)],
            *[pltpu.SemaphoreType.DMA((4, n)) for _ in range(2)],
            *[pltpu.SemaphoreType.DMA((4,)) for _ in range(2)],
            *[pltpu.SemaphoreType.DMA((32,)) for _ in range(2)],
        ],
        compiler_params=pltpu.CompilerParams(
            collective_id=0, has_side_effects=True, vmem_limit_bytes=56 * 2**20
        ),
    )(*taken)
    return out[0], out[1], out[2]


def solution(mesh):
    both = P(("row", "col"))
    in_specs = (P(None, ("row", "col")), both, both, both, both, P(), P(), P(), P(), P())
    return jax.shard_map(body, mesh=mesh, in_specs=in_specs, out_specs=(both, both, both), check_vma=False)
```

```python
import functools
import itertools
import math

import jax
import jax.numpy as jnp
from jax import lax
from jax.experimental import pallas as pl
from jax.experimental.pallas import tpu as pltpu
from jax.sharding import PartitionSpec as P

MESH = pl.DeviceIdType.MESH
F32 = jnp.float32
BF16 = jnp.bfloat16
LOG2E = math.log2(math.e)
MASKED = -2000.0
WIDTH = 256
PARTS = 1
SHIFTS = (2, 1, 3, 0)

PLAN = [
    ((0, 0, 0, 0), (0, 0, 0, 0)),
    ((0, 0, 0, 1), (0, 0, 0, 1)),
    ((0, 1, 0, 0), (0, 1, 0, 0)),
    ((-1, -1, 0, 0), (-1, -1, 0, 0)),
    ((-1, 0, -1, 0), (-1, 0, -1, 0)),
    ((1, 0, -1, 0), (1, 0, -1, 0)),
    ((1, 0, 1, 0), (1, 0, 1, 0)),
    ((-1, 0, -1, 1), (0, 0, 0, 1)),
    ((0, 2, 0, 0), (0, 1, 0, 0)),
    ((1, 0, -1, 1), (0, 0, 0, 1)),
    ((1, 1, 0, 0), (1, 0, 0, 0)),
    ((-1, 0, 2, 1), (0, 0, -1, 1)),
    ((-1, 2, 0, 0), (0, -1, 0, 0)),
    ((1, 0, 2, 0), (0, 0, 1, 0)),
    ((2, -1, 0, 1), (-1, 0, 0, 1)),
    ((-1, 2, 0, 1), (0, 0, 0, 1)),
]
OFFSETS = [row[0] for row in PLAN]


def diff(a, b):
    return ((a[0] - b[0]) % 4, (a[1] - b[1]) % 4, (a[2] - b[2]) % 4, (a[3] - b[3]) % 2)


HELD = [diff(block, (0, 0, 0, 0)) for block, _ in PLAN]
ORIGIN = [HELD.index(diff(block, sender)) for block, sender in PLAN]


def plan_units():
    seen, units = {(0, 0, 0, 0)}, [[] for _ in OFFSETS]
    units[0].append((0, 0, False))
    for a, b in sorted(itertools.combinations(range(len(OFFSETS)), 2), key=lambda p: p[1]):
        d, e = diff(OFFSETS[b], OFFSETS[a]), diff(OFFSETS[a], OFFSETS[b])
        if d in seen:
            continue
        seen.update((d, e))
        units[b].append((a, b, d != e))
    assert len(seen) == 128
    return units


UNITS = plan_units()
STEPS = [((), (0,))] + [((s,), (s,)) for s in range(1, 11)] + [((11, 12), (11,)), ((13, ), (12,)), ((14,), (13,)), ((15,), (14, 15))]


def place():
    r, c = lax.axis_index("row"), lax.axis_index("col")
    return c % 4, r // 4, (c // 4) * 2 + (r // 2) % 2, r % 2


def device_at(x, y, z, k):
    return ((y * 2 + z % 2) * 2 + k, (z // 2) * 4 + x)


def moved(me, offset, sign):
    x, y, z, k = me
    return device_at(
        (x + sign * offset[0] + 8) % 4,
        (y + sign * offset[1] + 4) % 4,
        (z + sign * offset[2] + 4) % 4,
        (k + offset[3]) % 2,
    )


def column_of(row, lanes):
    return jnp.broadcast_to(row, (lanes, row.shape[1])).T


def kernel(
    points_in,
    labels_in,
    solution_in,
    residual_in,
    direction_in,
    len_low_in,
    len_high_in,
    variances_in,
    nugget_in,
    coupling_in,
    out_ref,
    raw,
    aux,
    lhs,
    rhs,
    dir_col,
    dir_row,
    acc_col,
    acc_row,
    row_sum,
    part,
    back,
    own,
    sums,
    labels_ref,
    solution_ref,
    residual_ref,
    direction_ref,
    len_low_ref,
    len_high_ref,
    variances_ref,
    nugget_ref,
    coupling_ref,
    load_sem,
    send_sem,
    recv_sem,
    aux_send,
    aux_recv,
    back_send,
    back_recv,
    own_send,
    own_recv,
    sums_send,
    sums_recv,
):
    n = len(OFFSETS)
    me = place()
    x, y, z, k = me
    peers = []
    for j, l, kk in list(itertools.product(range(4), range(4), range(2)))[1:]:
        peers.append(device_at(x, (y + j) % 4, (z + l) % 4, (k + kk) % 2))

    targets = [moved(me, PLAN[s][1], -1) for s in range(1, n)]
    lines = [
        [moved(me, (dx + shift, dy, dz, dk), 1) for dx, dy, dz, dk in OFFSETS] for shift in range(4)
    ]

    barrier = pltpu.get_barrier_semaphore()
    near = sorted({row[1] for row in PLAN[1:]})
    greet = [moved(me, f, -1) for f in near] + [moved(me, f, 1) for f in near if diff(f, (0, 0, 0, 0)) != diff((0, 0, 0, 0), f)]
    for d in greet:
        pl.semaphore_signal(barrier, inc=1, device_id=d, device_id_type=MESH)

    pairs = [
        (labels_in, labels_ref),
        (direction_in, direction_ref),
        (points_in, raw.at[0]),
        (len_low_in, len_low_ref),
        (len_high_in, len_high_ref),
        (coupling_in, coupling_ref),
        (variances_in, variances_ref),
        (nugget_in, nugget_ref),
        (residual_in, residual_ref),
        (solution_in, solution_ref),
    ]
    loads = [pltpu.make_async_copy(src, dst, load_sem.at[i]) for i, (src, dst) in enumerate(pairs)]
    for load in loads:
        load.start()
    for load in loads[:2]:
        load.wait()
    lane = lax.broadcasted_iota(jnp.int32, (1, WIDTH), 1)
    fidelity = labels_ref[...].astype(F32)
    label = jnp.where(lane < 128, fidelity[:, 0:1], fidelity[:, 1:2])
    direction = direction_ref[...]
    aux[0] = jnp.concatenate([direction, label], axis=1)
    loads[2].wait()
    pl.semaphore_wait(barrier, len(greet))

    def copy_to(s, part_of):
        rows = pl.ds(part_of * (64 // PARTS), 64 // PARTS)
        return pltpu.make_async_remote_copy(
            src_ref=raw.at[ORIGIN[s], rows],
            dst_ref=raw.at[s, rows],
            send_sem=send_sem.at[s, part_of],
            recv_sem=recv_sem.at[s, part_of],
            device_id=targets[s - 1],
            device_id_type=MESH,
        )

    def aux_to(s):
        return pltpu.make_async_remote_copy(
            src_ref=aux.at[ORIGIN[s]],
            dst_ref=aux.at[s],
            send_sem=aux_send.at[s],
            recv_sem=aux_recv.at[s],
            device_id=targets[s - 1],
            device_id_type=MESH,
        )

    onward = [[s for s in range(1, n) if ORIGIN[s] == q] for q in range(n)]

    def pass_on(q, part_of):
        for s in onward[q]:
            copy_to(s, part_of).start()
            if part_of == 0:
                aux_to(s).start()

    def take(s):
        for part_of in range(PARTS):
            copy_to(s, part_of).wait_recv()
            if part_of == 0:
                aux_to(s).wait_recv()
            pass_on(s, part_of)

    for part_of in range(PARTS):
        pass_on(0, part_of)
    for load in loads[3:]:
        load.wait()

    root = math.sqrt(LOG2E)
    scales = [
        root / column_of(len_low_ref[...], 128),
        root / column_of(len_high_ref[...], 128),
    ]
    ones = jnp.ones((1, 128), F32)
    log_var = [0.5 * LOG2E * jnp.log(ones * variances_ref[0:1, 0:1]), 0.5 * LOG2E * jnp.log(ones * variances_ref[0:1, 1:2])]
    log_scale = LOG2E * jnp.log(ones * coupling_ref[...].reshape(1, 1))
    wide = lambda v: jnp.concatenate([v, v], axis=1)
    log_var = [wide(v) for v in log_var]
    log_scale = wide(log_scale)

    acc_col[...] = jnp.zeros_like(acc_col)
    acc_row[...] = jnp.zeros_like(acc_row)

    row16 = lax.broadcasted_iota(jnp.int32, (16, WIDTH), 0)
    zeros48 = jnp.zeros((48, WIDTH), BF16)

    def prepare(s, as_lhs, as_rhs):
        pts = raw[s]
        d = aux[s][:, :WIDTH]
        lab = aux[s][:, WIDTH:]
        for which in range(2):
            zz = pts * wide(scales[which])
            hi = zz.astype(BF16)
            hif = hi.astype(F32)
            lo = (zz - hif).astype(BF16)
            norm = jnp.sum(hif * (hif + 2.0 * lo.astype(F32)), axis=0, keepdims=True)
            extra = lab * log_scale if which == 0 else (1.0 - lab) * MASKED
            g = log_var[which] + extra - 0.5 * norm
            g1 = g.astype(BF16).astype(F32)
            g2 = (g - g1).astype(BF16).astype(F32)
            g3 = g - g1 - g2
            if as_lhs:
                e = jnp.where(row16 == 0, g1, jnp.where(row16 == 1, g2, jnp.where(row16 == 2, g3, 0.0)))
                e = jnp.where((row16 >= 3) & (row16 < 6), 1.0, e)
                full = jnp.concatenate([hi, hi, lo, e.astype(BF16), zeros48], axis=0)
                lhs[which, s] = full.T
            if as_rhs:
                e = jnp.where(row16 == 3, g1, jnp.where(row16 == 4, g2, jnp.where(row16 == 5, g3, 0.0)))
                e = jnp.where(row16 < 3, 1.0, e)
                rhs[which, s] = jnp.concatenate([hi, lo, hi, e.astype(BF16), zeros48], axis=0)
        dir_row[s] = jnp.broadcast_to(d, (8, WIDTH))
        if as_lhs:
            dir_col[s] = column_of(d, 128)

    def unit(a, b, both):
        el = jnp.dot(lhs[0, a], rhs[0, b], preferred_element_type=F32)
        eh = jnp.dot(lhs[1, a], rhs[1, b], preferred_element_type=F32)
        m = (jnp.exp2(el) + jnp.exp2(eh)).reshape(WIDTH // 8, 8, WIDTH)
        d = dir_col[a].reshape(WIDTH // 8, 8, 128)
        acc_col[b] += jnp.sum(m * jnp.concatenate([d, d], axis=2), axis=0)
        if both:
            t = m * dir_row[b][None]
            t = t[:, :, :128] + t[:, :, 128:]
            acc_row[a] += t.reshape(WIDTH, 128)

    flat = [u for us in UNITS for u in us]
    is_lhs = {a for a, _, _ in flat}
    is_rhs = {b for _, b, _ in flat}
    has_row = {a for a, _, both in flat if both}
    row_left = {a: sum(u[0] == a and u[2] for u in flat) for a in has_row}
    row_left.update({a: -1 for a in is_lhs - has_row})
    prepare(0, True, True)
    for taken, ready in STEPS:
        for s in taken:
            take(s)
        for s in taken:
            prepare(s, s in is_lhs, s in is_rhs)
        for u in sorted(u for s in ready for u in UNITS[s]):
            unit(*u)
            row_left[u[0]] -= u[2]
            if u[2] and row_left[u[0]] == 0:
                row_sum[u[0]] = jnp.sum(acc_row[u[0]].T, axis=0, keepdims=True)

    def total_of(s):
        t = jnp.zeros((1, WIDTH), F32)
        if s in is_rhs:
            t = t + jnp.sum(acc_col[s], axis=0, keepdims=True)
        if s in has_row:
            t = t + row_sum[s]
        return t

    def hand_back(s, shift):
        return pltpu.make_async_remote_copy(
            src_ref=part.at[s],
            dst_ref=back.at[shift, s],
            send_sem=back_send.at[shift, s],
            recv_sem=back_recv.at[shift, s],
            device_id=lines[shift][s],
            device_id_type=MESH,
        )

    def hand_own(shift):
        return pltpu.make_async_remote_copy(
            src_ref=own.at[0],
            dst_ref=own.at[shift],
            send_sem=own_send.at[shift],
            recv_sem=own_recv.at[shift],
            device_id=lines[shift][0],
            device_id_type=MESH,
        )

    residual = residual_ref[...]
    nugget_points = nugget_ref[0:1, 0:1] + (nugget_ref[0:1, 1:2] - nugget_ref[0:1, 0:1]) * label
    order = list(range(n - 1, 0, -1))
    for at, s in enumerate(order):
        part[s] = total_of(s)
        if at > 0:
            for shift in SHIFTS:
                hand_back(order[at - 1], shift).start()
    image = total_of(0) + nugget_points * direction
    own[0] = jnp.concatenate([image, residual, direction], axis=1)
    for shift in SHIFTS:
        hand_back(order[-1], shift).start()
    for shift in SHIFTS[:-1]:
        hand_own(shift).start()

    def fold(v):
        return v[:, :128] + v[:, 128:]

    total = jnp.zeros((4, 128), F32)
    for shift in (0, 1, 3, 2):
        if shift > 0:
            hand_own(shift).wait_recv()
        y_line, r_line, d_line = (own[shift][:, at * WIDTH : (at + 1) * WIDTH] for at in range(3))
        for s in order:
            hand_back(s, shift).wait_recv()
            y_line = y_line + back[shift, s]
        if shift == 0:
            image = y_line
        total = total + jnp.concatenate(
            [fold(r_line * r_line), fold(d_line * y_line), fold(r_line * y_line), fold(y_line * y_line)],
            axis=0,
        )
    sums[0] = total

    def send_sums(i):
        return pltpu.make_async_remote_copy(
            src_ref=sums.at[0],
            dst_ref=sums.at[i],
            send_sem=sums_send.at[i],
            recv_sem=sums_recv.at[i],
            device_id=peers[i - 1],
            device_id_type=MESH,
        )

    for i in range(31, 0, -1):
        send_sums(i).start()
    for i in range(1, 32):
        send_sums(i).wait_recv()
        total = total + sums[i]

    scal = jnp.sum(total, axis=1, keepdims=True)
    old_norm, curvature, cross, image_norm = scal[0:1], scal[1:2], scal[2:3], scal[3:4]
    step = old_norm / curvature
    new_norm = old_norm - 2.0 * step * cross + step * step * image_norm
    residual_next = residual - step * image
    out_ref[...] = jnp.concatenate(
        [
            solution_ref[...] + step * direction,
            residual_next,
            residual_next + new_norm / old_norm * direction,
        ],
        axis=0,
    )

    for s in range(1, n):
        for part_of in range(PARTS):
            copy_to(s, part_of).wait_send()
        aux_to(s).wait_send()
        for shift in SHIFTS:
            hand_back(s, shift).wait_send()
    for shift in SHIFTS[:-1]:
        hand_own(shift).wait_send()
    for i in range(1, 32):
        send_sums(i).wait_send()


def body(points, labels, solution, residual, direction, len_low, len_high, variances, nugget, coupling):
    n = len(OFFSETS)
    row = lambda v: v.reshape(1, v.shape[0])
    taken = [
        points,
        row(labels),
        row(solution),
        row(residual),
        row(direction),
        row(len_low),
        row(len_high),
        row(variances),
        row(nugget),
        coupling,
    ]
    small = taken[1:]
    out = pl.pallas_call(
        kernel,
        out_shape=jax.ShapeDtypeStruct((3, WIDTH), F32),
        in_specs=[pl.BlockSpec(memory_space=pl.ANY)] * len(taken),
        out_specs=pl.BlockSpec(memory_space=pltpu.VMEM),
        scratch_shapes=[
            pltpu.VMEM((n, 64, WIDTH), F32),
            pltpu.VMEM((n, 1, 2 * WIDTH), F32),
            pltpu.VMEM((2, n, WIDTH, WIDTH), BF16),
            pltpu.VMEM((2, n, WIDTH, WIDTH), BF16),
            pltpu.VMEM((n, WIDTH, 128), F32),
            pltpu.VMEM((n, 8, WIDTH), F32),
            pltpu.VMEM((n, 8, WIDTH), F32),
            pltpu.VMEM((n, WIDTH, 128), F32),
            pltpu.VMEM((n, 1, WIDTH), F32),
            pltpu.VMEM((n, 1, WIDTH), F32),
            pltpu.VMEM((4, n, 1, WIDTH), F32),
            pltpu.VMEM((4, 1, 3 * WIDTH), F32),
            pltpu.VMEM((32, 4, 128), F32),
            *[pltpu.VMEM(v.shape, v.dtype) for v in small],
            pltpu.SemaphoreType.DMA((len(taken),)),
            *[pltpu.SemaphoreType.DMA((n, PARTS)) for _ in range(2)],
            *[pltpu.SemaphoreType.DMA((n,)) for _ in range(2)],
            *[pltpu.SemaphoreType.DMA((4, n)) for _ in range(2)],
            *[pltpu.SemaphoreType.DMA((4,)) for _ in range(2)],
            *[pltpu.SemaphoreType.DMA((32,)) for _ in range(2)],
        ],
        compiler_params=pltpu.CompilerParams(
            collective_id=0, has_side_effects=True, vmem_limit_bytes=56 * 2**20
        ),
    )(*taken)
    return out[0], out[1], out[2]


def solution(mesh):
    both = P(("row", "col"))
    in_specs = (P(None, ("row", "col")), both, both, both, both, P(), P(), P(), P(), P())
    return jax.shard_map(body, mesh=mesh, in_specs=in_specs, out_specs=(both, both, both), check_vma=False)
```

```python
import functools
import itertools
import math

import jax
import jax.numpy as jnp
from jax import lax
from jax.experimental import pallas as pl
from jax.experimental.pallas import tpu as pltpu
from jax.sharding import PartitionSpec as P

MESH = pl.DeviceIdType.MESH
F32 = jnp.float32
BF16 = jnp.bfloat16
LOG2E = math.log2(math.e)
MASKED = -2000.0
WIDTH = 256
PARTS = 1
SHIFTS = (2, 1, 3, 0)

PLAN = [
    ((0, 0, 0, 0), (0, 0, 0, 0)),
    ((0, 0, 0, 1), (0, 0, 0, 1)),
    ((0, 1, 0, 0), (0, 1, 0, 0)),
    ((-1, -1, 0, 0), (-1, -1, 0, 0)),
    ((-1, 0, -1, 0), (-1, 0, -1, 0)),
    ((1, 0, -1, 0), (1, 0, -1, 0)),
    ((1, 0, 1, 0), (1, 0, 1, 0)),
    ((-1, 0, -1, 1), (0, 0, 0, 1)),
    ((0, 2, 0, 0), (0, 1, 0, 0)),
    ((1, 0, -1, 1), (0, 0, 0, 1)),
    ((1, 1, 0, 0), (1, 0, 0, 0)),
    ((-1, 0, 2, 1), (0, 0, -1, 1)),
    ((-1, 2, 0, 0), (0, -1, 0, 0)),
    ((1, 0, 2, 0), (0, 0, 1, 0)),
    ((2, -1, 0, 1), (-1, 0, 0, 1)),
    ((-1, 2, 0, 1), (0, 0, 0, 1)),
]
OFFSETS = [row[0] for row in PLAN]


def diff(a, b):
    return ((a[0] - b[0]) % 4, (a[1] - b[1]) % 4, (a[2] - b[2]) % 4, (a[3] - b[3]) % 2)


HELD = [diff(block, (0, 0, 0, 0)) for block, _ in PLAN]
ORIGIN = [HELD.index(diff(block, sender)) for block, sender in PLAN]


def plan_units():
    seen, units = {(0, 0, 0, 0)}, [[] for _ in OFFSETS]
    units[0].append((0, 0, False))
    for a, b in sorted(itertools.combinations(range(len(OFFSETS)), 2), key=lambda p: p[1]):
        d, e = diff(OFFSETS[b], OFFSETS[a]), diff(OFFSETS[a], OFFSETS[b])
        if d in seen:
            continue
        seen.update((d, e))
        units[b].append((a, b, d != e))
    assert len(seen) == 128
    return units


UNITS = plan_units()
STEPS = [((), (0,))] + [((s,), (s,)) for s in range(1, 11)] + [((11, 12), (11,)), ((13, ), (12,)), ((14,), (13,)), ((15,), (14, 15))]


def place():
    r, c = lax.axis_index("row"), lax.axis_index("col")
    return c % 4, r // 4, (c // 4) * 2 + (r // 2) % 2, r % 2


def device_at(x, y, z, k):
    return ((y * 2 + z % 2) * 2 + k, (z // 2) * 4 + x)


def moved(me, offset, sign):
    x, y, z, k = me
    return device_at(
        (x + sign * offset[0] + 8) % 4,
        (y + sign * offset[1] + 4) % 4,
        (z + sign * offset[2] + 4) % 4,
        (k + offset[3]) % 2,
    )


def column_of(row, lanes):
    return jnp.broadcast_to(row, (lanes, row.shape[1])).T


def kernel(
    points_in,
    labels_in,
    solution_in,
    residual_in,
    direction_in,
    len_low_in,
    len_high_in,
    variances_in,
    nugget_in,
    coupling_in,
    out_ref,
    raw,
    aux,
    lhs,
    rhs,
    dir_col,
    dir_row,
    acc_col,
    acc_row,
    row_sum,
    part,
    back,
    own,
    sums,
    labels_ref,
    solution_ref,
    residual_ref,
    direction_ref,
    len_low_ref,
    len_high_ref,
    variances_ref,
    nugget_ref,
    coupling_ref,
    load_sem,
    send_sem,
    recv_sem,
    aux_send,
    aux_recv,
    back_send,
    back_recv,
    own_send,
    own_recv,
    sums_send,
    sums_recv,
):
    n = len(OFFSETS)
    me = place()
    x, y, z, k = me
    peers = []
    for j, l, kk in list(itertools.product(range(4), range(4), range(2)))[1:]:
        peers.append(device_at(x, (y + j) % 4, (z + l) % 4, (k + kk) % 2))

    targets = [moved(me, PLAN[s][1], -1) for s in range(1, n)]
    lines = [
        [moved(me, (dx + shift, dy, dz, dk), 1) for dx, dy, dz, dk in OFFSETS] for shift in range(4)
    ]

    barrier = pltpu.get_barrier_semaphore()
    near = sorted({row[1] for row in PLAN[1:]})
    greet = [moved(me, f, -1) for f in near] + [moved(me, f, 1) for f in near if diff(f, (0, 0, 0, 0)) != diff((0, 0, 0, 0), f)]
    for d in greet:
        pl.semaphore_signal(barrier, inc=1, device_id=d, device_id_type=MESH)

    pairs = [
        (labels_in, labels_ref),
        (direction_in, direction_ref),
        (points_in, raw.at[0]),
        (len_low_in, len_low_ref),
        (len_high_in, len_high_ref),
        (coupling_in, coupling_ref),
        (variances_in, variances_ref),
        (nugget_in, nugget_ref),
        (residual_in, residual_ref),
        (solution_in, solution_ref),
    ]
    loads = [pltpu.make_async_copy(src, dst, load_sem.at[i]) for i, (src, dst) in enumerate(pairs)]
    for load in loads:
        load.start()
    for load in loads[:2]:
        load.wait()
    lane = lax.broadcasted_iota(jnp.int32, (1, WIDTH), 1)
    fidelity = labels_ref[...].astype(F32)
    label = jnp.where(lane < 128, fidelity[:, 0:1], fidelity[:, 1:2])
    direction = direction_ref[...]
    aux[0] = jnp.concatenate([direction, label], axis=1)
    loads[2].wait()
    pl.semaphore_wait(barrier, len(greet))

    def copy_to(s, part_of):
        rows = pl.ds(part_of * (64 // PARTS), 64 // PARTS)
        return pltpu.make_async_remote_copy(
            src_ref=raw.at[ORIGIN[s], rows],
            dst_ref=raw.at[s, rows],
            send_sem=send_sem.at[s, part_of],
            recv_sem=recv_sem.at[s, part_of],
            device_id=targets[s - 1],
            device_id_type=MESH,
        )

    def aux_to(s):
        return pltpu.make_async_remote_copy(
            src_ref=aux.at[ORIGIN[s]],
            dst_ref=aux.at[s],
            send_sem=aux_send.at[s],
            recv_sem=aux_recv.at[s],
            device_id=targets[s - 1],
            device_id_type=MESH,
        )

    onward = [[s for s in range(1, n) if ORIGIN[s] == q] for q in range(n)]

    def pass_on(q, part_of):
        for s in onward[q]:
            copy_to(s, part_of).start()
            if part_of == 0:
                aux_to(s).start()

    def take(s):
        for part_of in range(PARTS):
            copy_to(s, part_of).wait_recv()
            if part_of == 0:
                aux_to(s).wait_recv()
            pass_on(s, part_of)

    for part_of in range(PARTS):
        pass_on(0, part_of)
    for load in loads[3:]:
        load.wait()

    root = math.sqrt(LOG2E)
    scales = [
        root / column_of(len_low_ref[...], 128),
        root / column_of(len_high_ref[...], 128),
    ]
    ones = jnp.ones((1, 128), F32)
    log_var = [0.5 * LOG2E * jnp.log(ones * variances_ref[0:1, 0:1]), 0.5 * LOG2E * jnp.log(ones * variances_ref[0:1, 1:2])]
    log_scale = LOG2E * jnp.log(ones * coupling_ref[...].reshape(1, 1))
    wide = lambda v: jnp.concatenate([v, v], axis=1)
    log_var = [wide(v) for v in log_var]
    log_scale = wide(log_scale)

    acc_col[...] = jnp.zeros_like(acc_col)
    acc_row[...] = jnp.zeros_like(acc_row)

    row16 = lax.broadcasted_iota(jnp.int32, (16, WIDTH), 0)
    zeros48 = jnp.zeros((48, WIDTH), BF16)

    def prepare(s, as_lhs, as_rhs):
        pts = raw[s]
        d = aux[s][:, :WIDTH]
        lab = aux[s][:, WIDTH:]
        for which in range(2):
            zz = pts * wide(scales[which])
            hi = zz.astype(BF16)
            hif = hi.astype(F32)
            lo = (zz - hif).astype(BF16)
            norm = jnp.sum(hif * (hif + 2.0 * lo.astype(F32)), axis=0, keepdims=True)
            extra = lab * log_scale if which == 0 else (1.0 - lab) * MASKED
            g = log_var[which] + extra - 0.5 * norm
            g1 = g.astype(BF16).astype(F32)
            g2 = (g - g1).astype(BF16).astype(F32)
            g3 = g - g1 - g2
            if as_lhs:
                e = jnp.where(row16 == 0, g1, jnp.where(row16 == 1, g2, jnp.where(row16 == 2, g3, 0.0)))
                e = jnp.where((row16 >= 3) & (row16 < 6), 1.0, e)
                full = jnp.concatenate([hi, hi, lo, e.astype(BF16), zeros48], axis=0)
                lhs[which, s] = full.T
            if as_rhs:
                e = jnp.where(row16 == 3, g1, jnp.where(row16 == 4, g2, jnp.where(row16 == 5, g3, 0.0)))
                e = jnp.where(row16 < 3, 1.0, e)
                rhs[which, s] = jnp.concatenate([hi, lo, hi, e.astype(BF16), zeros48], axis=0)
        dir_row[s] = jnp.broadcast_to(d, (8, WIDTH))
        if as_lhs:
            dir_col[s] = column_of(d, 128)

    def unit(a, b, both):
        el = jnp.dot(lhs[0, a], rhs[0, b], preferred_element_type=F32)
        eh = jnp.dot(lhs[1, a], rhs[1, b], preferred_element_type=F32)
        m = (jnp.exp2(el) + jnp.exp2(eh)).reshape(WIDTH // 8, 8, WIDTH)
        d = dir_col[a].reshape(WIDTH // 8, 8, 128)
        acc_col[b] += jnp.sum(m * jnp.concatenate([d, d], axis=2), axis=0)
        if both:
            t = m * dir_row[b][None]
            t = t[:, :, :128] + t[:, :, 128:]
            acc_row[a] += t.reshape(WIDTH, 128)

    flat = [u for us in UNITS for u in us]
    is_lhs = {a for a, _, _ in flat}
    is_rhs = {b for _, b, _ in flat}
    has_row = {a for a, _, both in flat if both}
    def total_of(s):
        t = jnp.zeros((1, WIDTH), F32)
        if s in is_rhs:
            t = t + jnp.sum(acc_col[s], axis=0, keepdims=True)
        if s in has_row:
            t = t + row_sum[s]
        return t

    def hand_back(s, shift):
        return pltpu.make_async_remote_copy(
            src_ref=part.at[s],
            dst_ref=back.at[shift, s],
            send_sem=back_send.at[shift, s],
            recv_sem=back_recv.at[shift, s],
            device_id=lines[shift][s],
            device_id_type=MESH,
        )

    def hand_own(shift):
        return pltpu.make_async_remote_copy(
            src_ref=own.at[0],
            dst_ref=own.at[shift],
            send_sem=own_send.at[shift],
            recv_sem=own_recv.at[shift],
            device_id=lines[shift][0],
            device_id_type=MESH,
        )

    row_left = {a: sum(u[0] == a and u[2] for u in flat) for a in has_row}
    row_left.update({a: -1 for a in is_lhs - has_row})
    prepare(0, True, True)
    busy = {v for t in STEPS[-1][1] for u in UNITS[t] for v in u[:2]} | {0}
    early = [s for s in range(n - 1, 0, -1) if s not in busy]
    for at, (taken, ready) in enumerate(STEPS):
        if at == len(STEPS) - 1:
            for s in early:
                part[s] = total_of(s)
        for s in taken:
            take(s)
        for s in taken:
            prepare(s, s in is_lhs, s in is_rhs)
        if at == len(STEPS) - 1:
            for s in early:
                for shift in SHIFTS:
                    hand_back(s, shift).start()
        for u in sorted(u for s in ready for u in UNITS[s]):
            unit(*u)
            row_left[u[0]] -= u[2]
            if u[2] and row_left[u[0]] == 0:
                row_sum[u[0]] = jnp.sum(acc_row[u[0]].T, axis=0, keepdims=True)

    residual = residual_ref[...]
    nugget_points = nugget_ref[0:1, 0:1] + (nugget_ref[0:1, 1:2] - nugget_ref[0:1, 0:1]) * label
    order = [s for s in range(n - 1, 0, -1) if s not in early]
    for at, s in enumerate(order):
        part[s] = total_of(s)
        if at > 0:
            for shift in SHIFTS:
                hand_back(order[at - 1], shift).start()
    image = total_of(0) + nugget_points * direction
    own[0] = jnp.concatenate([image, residual, direction], axis=1)
    for shift in SHIFTS:
        hand_back(order[-1], shift).start()
    for shift in SHIFTS[:-1]:
        hand_own(shift).start()

    def fold(v):
        return v[:, :128] + v[:, 128:]

    total = jnp.zeros((4, 128), F32)
    for shift in (0, 1, 3, 2):
        if shift > 0:
            hand_own(shift).wait_recv()
        y_line, r_line, d_line = (own[shift][:, at * WIDTH : (at + 1) * WIDTH] for at in range(3))
        for s in early + order:
            hand_back(s, shift).wait_recv()
            y_line = y_line + back[shift, s]
        if shift == 0:
            image = y_line
        total = total + jnp.concatenate(
            [fold(r_line * r_line), fold(d_line * y_line), fold(r_line * y_line), fold(y_line * y_line)],
            axis=0,
        )
    sums[0] = total

    def send_sums(i):
        return pltpu.make_async_remote_copy(
            src_ref=sums.at[0],
            dst_ref=sums.at[i],
            send_sem=sums_send.at[i],
            recv_sem=sums_recv.at[i],
            device_id=peers[i - 1],
            device_id_type=MESH,
        )

    for i in range(31, 0, -1):
        send_sums(i).start()
    for i in range(1, 32):
        send_sums(i).wait_recv()
        total = total + sums[i]

    scal = jnp.sum(total, axis=1, keepdims=True)
    old_norm, curvature, cross, image_norm = scal[0:1], scal[1:2], scal[2:3], scal[3:4]
    step = old_norm / curvature
    new_norm = old_norm - 2.0 * step * cross + step * step * image_norm
    residual_next = residual - step * image
    out_ref[...] = jnp.concatenate(
        [
            solution_ref[...] + step * direction,
            residual_next,
            residual_next + new_norm / old_norm * direction,
        ],
        axis=0,
    )

    for s in range(1, n):
        for part_of in range(PARTS):
            copy_to(s, part_of).wait_send()
        aux_to(s).wait_send()
        for shift in SHIFTS:
            hand_back(s, shift).wait_send()
    for shift in SHIFTS[:-1]:
        hand_own(shift).wait_send()
    for i in range(1, 32):
        send_sums(i).wait_send()


def body(points, labels, solution, residual, direction, len_low, len_high, variances, nugget, coupling):
    n = len(OFFSETS)
    row = lambda v: v.reshape(1, v.shape[0])
    taken = [
        points,
        row(labels),
        row(solution),
        row(residual),
        row(direction),
        row(len_low),
        row(len_high),
        row(variances),
        row(nugget),
        coupling,
    ]
    small = taken[1:]
    out = pl.pallas_call(
        kernel,
        out_shape=jax.ShapeDtypeStruct((3, WIDTH), F32),
        in_specs=[pl.BlockSpec(memory_space=pl.ANY)] * len(taken),
        out_specs=pl.BlockSpec(memory_space=pltpu.VMEM),
        scratch_shapes=[
            pltpu.VMEM((n, 64, WIDTH), F32),
            pltpu.VMEM((n, 1, 2 * WIDTH), F32),
            pltpu.VMEM((2, n, WIDTH, WIDTH), BF16),
            pltpu.VMEM((2, n, WIDTH, WIDTH), BF16),
            pltpu.VMEM((n, WIDTH, 128), F32),
            pltpu.VMEM((n, 8, WIDTH), F32),
            pltpu.VMEM((n, 8, WIDTH), F32),
            pltpu.VMEM((n, WIDTH, 128), F32),
            pltpu.VMEM((n, 1, WIDTH), F32),
            pltpu.VMEM((n, 1, WIDTH), F32),
            pltpu.VMEM((4, n, 1, WIDTH), F32),
            pltpu.VMEM((4, 1, 3 * WIDTH), F32),
            pltpu.VMEM((32, 4, 128), F32),
            *[pltpu.VMEM(v.shape, v.dtype) for v in small],
            pltpu.SemaphoreType.DMA((len(taken),)),
            *[pltpu.SemaphoreType.DMA((n, PARTS)) for _ in range(2)],
            *[pltpu.SemaphoreType.DMA((n,)) for _ in range(2)],
            *[pltpu.SemaphoreType.DMA((4, n)) for _ in range(2)],
            *[pltpu.SemaphoreType.DMA((4,)) for _ in range(2)],
            *[pltpu.SemaphoreType.DMA((32,)) for _ in range(2)],
        ],
        compiler_params=pltpu.CompilerParams(
            collective_id=0, has_side_effects=True, vmem_limit_bytes=56 * 2**20
        ),
    )(*taken)
    return out[0], out[1], out[2]


def solution(mesh):
    both = P(("row", "col"))
    in_specs = (P(None, ("row", "col")), both, both, both, both, P(), P(), P(), P(), P())
    return jax.shard_map(body, mesh=mesh, in_specs=in_specs, out_specs=(both, both, both), check_vma=False)
```

```python
import functools
import itertools
import math

import jax
import jax.numpy as jnp
from jax import lax
from jax.experimental import pallas as pl
from jax.experimental.pallas import tpu as pltpu
from jax.sharding import PartitionSpec as P

MESH = pl.DeviceIdType.MESH
F32 = jnp.float32
BF16 = jnp.bfloat16
LOG2E = math.log2(math.e)
MASKED = -2000.0
WIDTH = 256
PARTS = 1
SHIFTS = (2, 1, 3, 0)

PLAN = [
    ((0, 0, 0, 0), (0, 0, 0, 0)),
    ((0, 0, 0, 1), (0, 0, 0, 1)),
    ((0, 1, 0, 0), (0, 1, 0, 0)),
    ((-1, -1, 0, 0), (-1, -1, 0, 0)),
    ((-1, 0, -1, 0), (-1, 0, -1, 0)),
    ((1, 0, -1, 0), (1, 0, -1, 0)),
    ((1, 0, 1, 0), (1, 0, 1, 0)),
    ((-1, 0, -1, 1), (0, 0, 0, 1)),
    ((0, 2, 0, 0), (0, 1, 0, 0)),
    ((1, 0, -1, 1), (0, 0, 0, 1)),
    ((1, 1, 0, 0), (1, 0, 0, 0)),
    ((-1, 0, 2, 1), (0, 0, -1, 1)),
    ((-1, 2, 0, 0), (0, -1, 0, 0)),
    ((1, 0, 2, 0), (0, 0, 1, 0)),
    ((2, -1, 0, 1), (-1, 0, 0, 1)),
    ((-1, 2, 0, 1), (0, 0, 0, 1)),
]
OFFSETS = [row[0] for row in PLAN]


def diff(a, b):
    return ((a[0] - b[0]) % 4, (a[1] - b[1]) % 4, (a[2] - b[2]) % 4, (a[3] - b[3]) % 2)


HELD = [diff(block, (0, 0, 0, 0)) for block, _ in PLAN]
ORIGIN = [HELD.index(diff(block, sender)) for block, sender in PLAN]


def plan_units():
    seen, units = {(0, 0, 0, 0)}, [[] for _ in OFFSETS]
    units[0].append((0, 0, False))
    for a, b in sorted(itertools.combinations(range(len(OFFSETS)), 2), key=lambda p: p[1]):
        d, e = diff(OFFSETS[b], OFFSETS[a]), diff(OFFSETS[a], OFFSETS[b])
        if d in seen:
            continue
        seen.update((d, e))
        units[b].append((a, b, d != e))
    assert len(seen) == 128
    return units


UNITS = plan_units()
STEPS = [((), (0,))] + [((s,), (s,)) for s in range(1, 11)] + [((11, 12), (11,)), ((13, ), (12,)), ((14,), (13,)), ((15,), (14, 15))]


def place():
    r, c = lax.axis_index("row"), lax.axis_index("col")
    return c % 4, r // 4, (c // 4) * 2 + (r // 2) % 2, r % 2


def device_at(x, y, z, k):
    return ((y * 2 + z % 2) * 2 + k, (z // 2) * 4 + x)


def moved(me, offset, sign):
    x, y, z, k = me
    return device_at(
        (x + sign * offset[0] + 8) % 4,
        (y + sign * offset[1] + 4) % 4,
        (z + sign * offset[2] + 4) % 4,
        (k + offset[3]) % 2,
    )


def column_of(row, lanes):
    return jnp.broadcast_to(row, (lanes, row.shape[1])).T


def kernel(
    points_in,
    labels_in,
    solution_in,
    residual_in,
    direction_in,
    len_low_in,
    len_high_in,
    variances_in,
    nugget_in,
    coupling_in,
    out_ref,
    raw,
    aux,
    lhs,
    rhs,
    dir_col,
    dir_row,
    acc_col,
    acc_row,
    row_sum,
    part,
    back,
    own,
    sums,
    labels_ref,
    solution_ref,
    residual_ref,
    direction_ref,
    len_low_ref,
    len_high_ref,
    variances_ref,
    nugget_ref,
    coupling_ref,
    load_sem,
    send_sem,
    recv_sem,
    aux_send,
    aux_recv,
    back_send,
    back_recv,
    own_send,
    own_recv,
    sums_send,
    sums_recv,
):
    n = len(OFFSETS)
    me = place()
    x, y, z, k = me
    peers = []
    for j, l, kk in list(itertools.product(range(4), range(4), range(2)))[1:]:
        peers.append(device_at(x, (y + j) % 4, (z + l) % 4, (k + kk) % 2))

    targets = [moved(me, PLAN[s][1], -1) for s in range(1, n)]
    lines = [
        [moved(me, (dx + shift, dy, dz, dk), 1) for dx, dy, dz, dk in OFFSETS] for shift in range(4)
    ]

    barrier = pltpu.get_barrier_semaphore()
    near = sorted({row[1] for row in PLAN[1:]})
    greet = [moved(me, f, -1) for f in near] + [moved(me, f, 1) for f in near if diff(f, (0, 0, 0, 0)) != diff((0, 0, 0, 0), f)]
    for d in greet:
        pl.semaphore_signal(barrier, inc=1, device_id=d, device_id_type=MESH)

    pairs = [
        (labels_in, labels_ref),
        (direction_in, direction_ref),
        (points_in, raw.at[0]),
        (len_low_in, len_low_ref),
        (len_high_in, len_high_ref),
        (coupling_in, coupling_ref),
        (variances_in, variances_ref),
        (nugget_in, nugget_ref),
        (residual_in, residual_ref),
        (solution_in, solution_ref),
    ]
    loads = [pltpu.make_async_copy(src, dst, load_sem.at[i]) for i, (src, dst) in enumerate(pairs)]
    for load in loads:
        load.start()
    for load in loads[:2]:
        load.wait()
    lane = lax.broadcasted_iota(jnp.int32, (1, WIDTH), 1)
    fidelity = labels_ref[...].astype(F32)
    label = jnp.where(lane < 128, fidelity[:, 0:1], fidelity[:, 1:2])
    direction = direction_ref[...]
    aux[0] = jnp.concatenate([direction, label], axis=1)
    loads[2].wait()
    pl.semaphore_wait(barrier, len(greet))

    def copy_to(s, part_of):
        rows = pl.ds(part_of * (64 // PARTS), 64 // PARTS)
        return pltpu.make_async_remote_copy(
            src_ref=raw.at[ORIGIN[s], rows],
            dst_ref=raw.at[s, rows],
            send_sem=send_sem.at[s, part_of],
            recv_sem=recv_sem.at[s, part_of],
            device_id=targets[s - 1],
            device_id_type=MESH,
        )

    def aux_to(s):
        return pltpu.make_async_remote_copy(
            src_ref=aux.at[ORIGIN[s]],
            dst_ref=aux.at[s],
            send_sem=aux_send.at[s],
            recv_sem=aux_recv.at[s],
            device_id=targets[s - 1],
            device_id_type=MESH,
        )

    onward = [[s for s in range(1, n) if ORIGIN[s] == q] for q in range(n)]

    def pass_on(q, part_of):
        for s in onward[q]:
            copy_to(s, part_of).start()
            if part_of == 0:
                aux_to(s).start()

    def take(s):
        for part_of in range(PARTS):
            copy_to(s, part_of).wait_recv()
            if part_of == 0:
                aux_to(s).wait_recv()
            pass_on(s, part_of)

    for part_of in range(PARTS):
        pass_on(0, part_of)
    for load in loads[3:]:
        load.wait()

    root = math.sqrt(LOG2E)
    scales = [
        root / column_of(len_low_ref[...], 128),
        root / column_of(len_high_ref[...], 128),
    ]
    ones = jnp.ones((1, 128), F32)
    log_var = [0.5 * LOG2E * jnp.log(ones * variances_ref[0:1, 0:1]), 0.5 * LOG2E * jnp.log(ones * variances_ref[0:1, 1:2])]
    log_scale = LOG2E * jnp.log(ones * coupling_ref[...].reshape(1, 1))
    wide = lambda v: jnp.concatenate([v, v], axis=1)
    log_var = [wide(v) for v in log_var]
    log_scale = wide(log_scale)

    acc_col[...] = jnp.zeros_like(acc_col)
    acc_row[...] = jnp.zeros_like(acc_row)

    row16 = lax.broadcasted_iota(jnp.int32, (16, WIDTH), 0)
    zeros48 = jnp.zeros((48, WIDTH), BF16)

    def prepare(s, as_lhs, as_rhs):
        pts = raw[s]
        d = aux[s][:, :WIDTH]
        lab = aux[s][:, WIDTH:]
        for which in range(2):
            zz = pts * wide(scales[which])
            hi = zz.astype(BF16)
            hif = hi.astype(F32)
            lo = (zz - hif).astype(BF16)
            norm = jnp.sum(hif * (hif + 2.0 * lo.astype(F32)), axis=0, keepdims=True)
            extra = lab * log_scale if which == 0 else (1.0 - lab) * MASKED
            g = log_var[which] + extra - 0.5 * norm
            g1 = g.astype(BF16).astype(F32)
            g2 = (g - g1).astype(BF16).astype(F32)
            g3 = g - g1 - g2
            if as_lhs:
                e = jnp.where(row16 == 0, g1, jnp.where(row16 == 1, g2, jnp.where(row16 == 2, g3, 0.0)))
                e = jnp.where((row16 >= 3) & (row16 < 6), 1.0, e)
                full = jnp.concatenate([hi, hi, lo, e.astype(BF16), zeros48], axis=0)
                lhs[which, s] = full.T
            if as_rhs:
                e = jnp.where(row16 == 3, g1, jnp.where(row16 == 4, g2, jnp.where(row16 == 5, g3, 0.0)))
                e = jnp.where(row16 < 3, 1.0, e)
                rhs[which, s] = jnp.concatenate([hi, lo, hi, e.astype(BF16), zeros48], axis=0)
        dir_row[s] = jnp.broadcast_to(d, (8, WIDTH))
        if as_lhs:
            dir_col[s] = column_of(d, 128)

    def unit(a, b, both):
        el = jnp.dot(lhs[0, a], rhs[0, b], preferred_element_type=F32)
        eh = jnp.dot(lhs[1, a], rhs[1, b], preferred_element_type=F32)
        m = (jnp.exp2(el) + jnp.exp2(eh)).reshape(WIDTH // 8, 8, WIDTH)
        d = dir_col[a].reshape(WIDTH // 8, 8, 128)
        acc_col[b] += jnp.sum(m * jnp.concatenate([d, d], axis=2), axis=0)
        if both:
            t = m * dir_row[b][None]
            t = t[:, :, :128] + t[:, :, 128:]
            acc_row[a] += t.reshape(WIDTH, 128)

    flat = [u for us in UNITS for u in us]
    is_lhs = {a for a, _, _ in flat}
    is_rhs = {b for _, b, _ in flat}
    has_row = {a for a, _, both in flat if both}
    def total_of(s):
        t = jnp.zeros((1, WIDTH), F32)
        if s in is_rhs:
            t = t + jnp.sum(acc_col[s], axis=0, keepdims=True)
        if s in has_row:
            t = t + row_sum[s]
        return t

    def hand_back(s, shift):
        return pltpu.make_async_remote_copy(
            src_ref=part.at[s],
            dst_ref=back.at[shift, s],
            send_sem=back_send.at[shift, s],
            recv_sem=back_recv.at[shift, s],
            device_id=lines[shift][s],
            device_id_type=MESH,
        )

    def hand_own(shift):
        return pltpu.make_async_remote_copy(
            src_ref=own.at[0],
            dst_ref=own.at[shift],
            send_sem=own_send.at[shift],
            recv_sem=own_recv.at[shift],
            device_id=lines[shift][0],
            device_id_type=MESH,
        )

    row_left = {a: sum(u[0] == a and u[2] for u in flat) for a in has_row}
    row_left.update({a: -1 for a in is_lhs - has_row})
    prepare(0, True, True)
    busy = {v for t in STEPS[-1][1] for u in UNITS[t] for v in u[:2]} | {0}
    early = [s for s in range(n - 1, 0, -1) if s not in busy]
    for at, (taken, ready) in enumerate(STEPS):
        if at == len(STEPS) - 1:
            for s in early:
                part[s] = total_of(s)
        for s in taken:
            take(s)
        for s in taken:
            prepare(s, s in is_lhs, s in is_rhs)
        if at == len(STEPS) - 1:
            for s in early:
                for shift in SHIFTS:
                    hand_back(s, shift).start()
        for u in sorted(u for s in ready for u in UNITS[s]):
            unit(*u)
            row_left[u[0]] -= u[2]
            if u[2] and row_left[u[0]] == 0:
                row_sum[u[0]] = jnp.sum(acc_row[u[0]].T, axis=0, keepdims=True)

    residual = residual_ref[...]
    nugget_points = nugget_ref[0:1, 0:1] + (nugget_ref[0:1, 1:2] - nugget_ref[0:1, 0:1]) * label
    order = [s for s in range(n - 1, 0, -1) if s not in early]
    for at, s in enumerate(order):
        part[s] = total_of(s)
        if at > 0:
            for shift in SHIFTS:
                hand_back(order[at - 1], shift).start()
    image = total_of(0) + nugget_points * direction
    own[0] = jnp.concatenate([image, residual, direction], axis=1)
    for shift in SHIFTS:
        hand_back(order[-1], shift).start()
    for shift in SHIFTS[:-1]:
        hand_own(shift).start()

    def fold(v):
        return v[:, :128] + v[:, 128:]

    total = jnp.zeros((4, 128), F32)
    for shift in (0, 1, 3, 2):
        if shift > 0:
            hand_own(shift).wait_recv()
        y_line, r_line, d_line = (own[shift][:, at * WIDTH : (at + 1) * WIDTH] for at in range(3))
        for s in early + order:
            hand_back(s, shift).wait_recv()
            y_line = y_line + back[shift, s]
        if shift == 0:
            image = y_line
        total = total + jnp.concatenate(
            [fold(r_line * r_line), fold(d_line * y_line), fold(r_line * y_line), fold(y_line * y_line)],
            axis=0,
        )
    sums[0] = total

    def send_sums(i):
        return pltpu.make_async_remote_copy(
            src_ref=sums.at[0],
            dst_ref=sums.at[i],
            send_sem=sums_send.at[i],
            recv_sem=sums_recv.at[i],
            device_id=peers[i - 1],
            device_id_type=MESH,
        )

    for i in range(31, 0, -1):
        send_sums(i).start()
    for i in range(1, 32):
        send_sums(i).wait_recv()
        total = total + sums[i]

    scal = jnp.sum(total, axis=1, keepdims=True)
    old_norm, curvature, cross, image_norm = scal[0:1], scal[1:2], scal[2:3], scal[3:4]
    step = old_norm / curvature
    new_norm = old_norm - 2.0 * step * cross + step * step * image_norm
    residual_next = residual - step * image
    out_ref[...] = jnp.concatenate(
        [
            solution_ref[...] + step * direction,
            residual_next,
            residual_next + new_norm / old_norm * direction,
        ],
        axis=0,
    )

    for s in range(1, n):
        for part_of in range(PARTS):
            copy_to(s, part_of).wait_send()
        aux_to(s).wait_send()
        for shift in SHIFTS:
            hand_back(s, shift).wait_send()
    for shift in SHIFTS[:-1]:
        hand_own(shift).wait_send()
    for i in range(1, 32):
        send_sums(i).wait_send()


def body(points, labels, solution, residual, direction, len_low, len_high, variances, nugget, coupling):
    n = len(OFFSETS)
    row = lambda v: v.reshape(1, v.shape[0])
    taken = [
        points,
        row(labels),
        row(solution),
        row(residual),
        row(direction),
        row(len_low),
        row(len_high),
        row(variances),
        row(nugget),
        coupling,
    ]
    small = taken[1:]
    out = pl.pallas_call(
        kernel,
        out_shape=jax.ShapeDtypeStruct((3, WIDTH), F32),
        in_specs=[pl.BlockSpec(memory_space=pl.ANY)] * len(taken),
        out_specs=pl.BlockSpec(memory_space=pltpu.VMEM),
        scratch_shapes=[
            pltpu.VMEM((n, 64, WIDTH), F32),
            pltpu.VMEM((n, 1, 2 * WIDTH), F32),
            pltpu.VMEM((2, n, WIDTH, WIDTH), BF16),
            pltpu.VMEM((2, n, WIDTH, WIDTH), BF16),
            pltpu.VMEM((n, WIDTH, 128), F32),
            pltpu.VMEM((n, 8, WIDTH), F32),
            pltpu.VMEM((n, 8, WIDTH), F32),
            pltpu.VMEM((n, WIDTH, 128), F32),
            pltpu.VMEM((n, 1, WIDTH), F32),
            pltpu.VMEM((n, 1, WIDTH), F32),
            pltpu.VMEM((4, n, 1, WIDTH), F32),
            pltpu.VMEM((4, 1, 3 * WIDTH), F32),
            pltpu.VMEM((32, 4, 128), F32),
            *[pltpu.VMEM(v.shape, v.dtype) for v in small],
            pltpu.SemaphoreType.DMA((len(taken),)),
            *[pltpu.SemaphoreType.DMA((n, PARTS)) for _ in range(2)],
            *[pltpu.SemaphoreType.DMA((n,)) for _ in range(2)],
            *[pltpu.SemaphoreType.DMA((4, n)) for _ in range(2)],
            *[pltpu.SemaphoreType.DMA((4,)) for _ in range(2)],
            *[pltpu.SemaphoreType.DMA((32,)) for _ in range(2)],
        ],
        compiler_params=pltpu.CompilerParams(
            collective_id=0, has_side_effects=True, vmem_limit_bytes=28 * 2**20
        ),
    )(*taken)
    return out[0], out[1], out[2]


def solution(mesh):
    both = P(("row", "col"))
    in_specs = (P(None, ("row", "col")), both, both, both, both, P(), P(), P(), P(), P())
    return jax.shard_map(body, mesh=mesh, in_specs=in_specs, out_specs=(both, both, both), check_vma=False)
```
